64 devices in a mesh: rep: 4 (over x, y), dp: 16 (over z, core).
Axes of the slice: x: 2, y: 2, z: 8, core: 2. Of those that a mesh axis runs over, the one named last changes fastest.
The devices are a block of a 4x4x8 slice.
Arguments:
- x: bfloat16 [64, 4096, 512], P(('rep', 'dp')), parts along dimension 0
- dy: bfloat16 [64, 4096, 512], P(('rep', 'dp')), parts along dimension 0
- w_gate: bfloat16 [2, 512, 1408], P(None, 'dp')
- w_up: bfloat16 [2, 512, 1408], P(None, 'dp')
- w_down: bfloat16 [2, 1408, 512], P(None, 'dp')
- m_w_gate: float32 [2, 512, 1408], P(None, 'dp')
- m_w_up: float32 [2, 512, 1408], P(None, 'dp')
- m_w_down: float32 [2, 1408, 512], P(None, 'dp')
- v_w_gate: float32 [2, 512, 1408], P(None, 'dp')
- v_w_up: float32 [2, 512, 1408], P(None, 'dp')
- v_w_down: float32 [2, 1408, 512], P(None, 'dp')
Outputs:
- output 1: bfloat16 [8, 512, 1408], P('rep', 'dp'), parts along dimension 0
- output 2: bfloat16 [8, 512, 1408], P('rep', 'dp'), parts along dimension 0
- output 3: bfloat16 [8, 1408, 512], P('rep', 'dp'), parts along dimension 0
- output 4: float32 [8, 512, 1408], P('rep', 'dp'), parts along dimension 0
- output 5: float32 [8, 512, 1408], P('rep', 'dp'), parts along dimension 0
- output 6: float32 [8, 1408, 512], P('rep', 'dp'), parts along dimension 0
- output 7: float32 [8, 512, 1408], P('rep', 'dp'), parts along dimension 0
- output 8: float32 [8, 512, 1408], P('rep', 'dp'), parts along dimension 0
- output 9: float32 [8, 1408, 512], P('rep', 'dp'), parts along dimension 0
There are 4 independent parts. The reference program is written for one: setup_inputs(seed, part) draws one part's arguments, and reference() takes and returns one part's arrays. A program takes and returns all parts, laid end to end along the dimension named above; an argument that names none is the same for every part.
All inputs are finite; a program needn't handle non-finite values.
Results may differ from the reference program's by a relative error of at most 0.0225.
Values are sent between devices in bfloat16 or wider.
A program may use at most 768 MiB of HBM per device.

```python
import jax
import jax.numpy as jnp
from jax import lax

SEQUENCES = 16
TOKENS = 4096
D = 512
FF = 1408
LAYERS = 2
NAMES = ("w_gate", "w_up", "w_down")
SHAPES = {"w_gate": (LAYERS, D, FF), "w_up": (LAYERS, D, FF), "w_down": (LAYERS, FF, D)}


def bump(key, n, height):
    away = (jnp.arange(n, dtype=jnp.int32) - jax.random.randint(key, (), 0, n, jnp.int32)) % n
    return jnp.where(away < n // 8, height, 1.0)


def together(key, own, strength):
    shared = jax.random.normal(key, own.shape[1:], jnp.float32)
    return (own + strength * shared) * lax.rsqrt(1 + strength * strength)


def setup_inputs(seed: int = 0, part: int = 0) -> dict:
    kx, kdy, ka, kb, kz, kf, kh, kl, *keys = jax.random.split(jax.random.key(seed), 8 + 3 * len(NAMES))
    kx, kdy, ka, kb = (jax.random.fold_in(k, part) for k in (kx, kdy, ka, kb))
    kw, km, kv = (keys[i::3] for i in range(3))
    shape = (SEQUENCES, TOKENS, D)
    much_x, much_dy = jax.random.uniform(kz, (2,), jnp.float32, 0.0, 1.0)
    loud = 2.0 ** jax.random.uniform(jax.random.fold_in(kz, 1), (), jnp.float32, -1.0, 2.0)
    layers = 2.0 ** jax.random.uniform(kl, (LAYERS, 1, 1), jnp.float32, -1.0, 1.0)
    x = together(ka, jax.random.normal(kx, shape, jnp.float32), much_x) * bump(kf, D, 4.0)
    dy = together(kb, jax.random.normal(kdy, shape, jnp.float32), much_dy)
    drawn = {"x": x.astype(jnp.bfloat16), "dy": (loud * dy * (SEQUENCES * TOKENS) ** -0.5).astype(jnp.bfloat16)}
    for key, name in zip(kw, NAMES, strict=True):
        w = jax.random.normal(key, SHAPES[name], jnp.float32) * SHAPES[name][1] ** -0.5
        drawn[name] = (w * {"w_gate": 1.0, "w_up": bump(kh, FF, 4.0), "w_down": layers}[name]).astype(jnp.bfloat16)
    for key, name in zip(km, NAMES, strict=True):
        drawn[f"m_{name}"] = 0.1 * jax.random.normal(key, SHAPES[name], jnp.float32)
    for key, name in zip(kv, NAMES, strict=True):
        drawn[f"v_{name}"] = jax.random.uniform(key, SHAPES[name], jnp.float32, 0.005, 0.015)
    return drawn


def matmul(a, w):
    return jnp.dot(a, w, preferred_element_type=jnp.float32).astype(jnp.bfloat16)


def normed(h):
    wide = h.astype(jnp.float32)
    scale = lax.rsqrt(jnp.mean(wide**2, -1, keepdims=True) + 1e-6)
    return (wide * scale).astype(jnp.bfloat16)


def layer(h, w):
    a = normed(h)
    gate = jnp.dot(a, w["w_gate"], preferred_element_type=jnp.float32)
    up = jnp.dot(a, w["w_up"], preferred_element_type=jnp.float32)
    return h + matmul((jax.nn.silu(gate) * up).astype(jnp.bfloat16), w["w_down"])


def adamw(w, m, v, g):
    m = 0.9 * m + 0.1 * g
    v = 0.95 * v + 0.05 * g * g
    step = m * lax.rsqrt(v + 1e-8) + 0.1 * w
    return (w - 0.02 * step).astype(jnp.bfloat16), m, v


def clipped(gradients, sum_of_squares, count):
    factor = jnp.minimum(1.0, 0.5 * lax.rsqrt(sum_of_squares / count + 1e-30))
    return [g * factor for g in gradients]


def stack(weights, h):
    return lax.scan(lambda h, w: (layer(h, w), None), h, weights)[0]


def reference(x, dy, w_gate, w_up, w_down, m_w_gate, m_w_up, m_w_down, v_w_gate, v_w_up, v_w_down):
    weights = dict(zip(NAMES, (w_gate, w_up, w_down), strict=True))

    def take(so_far, sequence):
        h, by_y = sequence
        _, back = jax.vjp(lambda w: stack(w, h), weights)
        return jax.tree.map(lambda total, term: total + term.astype(jnp.float32), so_far, back(by_y)[0]), None

    none_yet = {name: jnp.zeros(w.shape, jnp.float32) for name, w in weights.items()}
    by_weights, _ = lax.scan(take, none_yet, (x, dy))
    gradients = [by_weights[name].astype(jnp.bfloat16).astype(jnp.float32) for name in NAMES]
    gradients = clipped(gradients, sum(jnp.sum(g * g) for g in gradients), sum(g.size for g in gradients))
    new = [
        adamw(w.astype(jnp.float32), m, v, g)
        for w, m, v, g in zip((w_gate, w_up, w_down), (m_w_gate, m_w_up, m_w_down), (v_w_gate, v_w_up, v_w_down), gradients, strict=True)
    ]
    return tuple(one[which] for which in range(3) for one in new)
```

```python
import functools

import jax
import jax.numpy as jnp
from jax import lax
from jax.experimental import pallas as pl
from jax.experimental.pallas import tpu as pltpu
from jax.sharding import PartitionSpec as P

F32, BF16 = jnp.float32, jnp.bfloat16
TILE = 512
VMEM_LIMIT = 60 << 20
MESH = pl.DeviceIdType.MESH


def dot(a, b):
    return jnp.dot(a, b, preferred_element_type=F32)


def norm_parts(h):
    wide = h.astype(F32)
    scale = lax.rsqrt(jnp.mean(wide * wide, -1, keepdims=True) + 1e-6)
    return wide, scale, (wide * scale).astype(BF16)


def sigmoid(x):
    return 0.5 * jnp.tanh(0.5 * x) + 0.5


class Place:
    def __init__(self, chips):
        me = lax.axis_index("dp")
        self.chips, self.half = chips, chips // 2
        self.z, self.c = me // 2, me % 2
        self.sibling = self.z * 2 + 1 - self.c

    def chip(self, offset):
        return lax.rem(self.z + offset + 2 * self.chips, self.chips)

    def beside(self, direction):
        return self.chip(direction) * 2 + self.c


def meet(devices):
    barrier = pltpu.get_barrier_semaphore()
    for device in devices:
        pl.semaphore_signal(barrier, inc=1, device_id={"dp": device}, device_id_type=MESH)
    pl.semaphore_wait(barrier, len(devices))


def remote(src, dst, send, recv, device):
    return pltpu.make_async_remote_copy(src_ref=src, dst_ref=dst, send_sem=send, recv_sem=recv, device_id={"dp": device}, device_id_type=MESH)


DIRECTIONS = (1, -1)


class Gather:
    def __init__(self, place, shards, fulls, signs, ring_send, ring_recv, side_send, side_recv, own_sem):
        self.p, self.shards, self.fulls, self.signs = place, shards, fulls, signs
        self.sems = (ring_send, ring_recv, side_send, side_recv, own_sem)

    @staticmethod
    def scratch(chips, matrices):
        ring, side = 2 * (chips // 2) * matrices, (2 * (chips // 2) + 1) * matrices
        dma = pltpu.SemaphoreType.DMA
        return [dma((ring,)), dma((ring,)), dma((side,)), dma((side,)), dma((matrices,))]

    def goes(self, direction, step, m):
        return step < self.p.half - 1 or self.signs[m] == direction

    def ring(self, direction, step, m):
        p, k = self.p, ((direction < 0) * self.p.half + step) * len(self.fulls) + m
        place = self.fulls[m].at[p.chip(-direction * step), p.c]
        return remote(self.shards[m] if step == 0 else place, place, self.sems[0].at[k], self.sems[1].at[k], p.beside(direction))

    def side(self, direction, step, m):
        p, n = self.p, len(self.fulls)
        k = (0 if step == 0 else 1 + (direction < 0) * p.half + step - 1) * n + m
        place = self.fulls[m].at[p.chip(-direction * step), p.c]
        return remote(self.shards[m] if step == 0 else place, place, self.sems[2].at[k], self.sems[3].at[k], p.sibling)

    def own(self, m):
        return pltpu.make_async_copy(self.shards[m], self.fulls[m].at[self.p.z, self.p.c], self.sems[4].at[m])

    def step(self, step):
        matrices = range(len(self.fulls))
        for m in matrices:
            for direction in DIRECTIONS:
                if step > 0 and self.goes(direction, step - 1, m):
                    self.ring(direction, step - 1, m).wait_recv()
                if step < self.p.half and self.goes(direction, step, m):
                    self.ring(direction, step, m).start()
                if step > 0 and self.goes(direction, step - 1, m):
                    self.side(direction, step, m).start()
            if step == 0:
                self.side(1, 0, m).start()
                self.own(m).start()

    def finish(self):
        for m in range(len(self.fulls)):
            self.own(m).wait()
            self.side(1, 0, m).wait()
            for direction in DIRECTIONS:
                for step in range(self.p.half):
                    if self.goes(direction, step, m):
                        self.ring(direction, step, m).wait_send()
                        self.side(direction, step + 1, m).wait()


class Scatter:
    def __init__(self, place, terms, signs, scratch):
        self.p, self.terms, self.signs, n = place, terms, signs, len(terms)
        self.own, self.other, self.sent, self.came = (scratch[i * n : (i + 1) * n] for i in range(4))
        self.own_sem, self.pair_send, self.pair_recv, self.ring_send, self.ring_recv = scratch[4 * n :]

    @staticmethod
    def scratch(chips, shapes):
        steps, n, dma = chips // 2, len(shapes), pltpu.SemaphoreType.DMA
        blocks = [pltpu.VMEM((chips, *shape), BF16) for shape in shapes]
        slots = [pltpu.VMEM((2 * steps, *shape), BF16) for shape in shapes]
        return blocks * 2 + slots * 2 + [dma((n,)), dma((n,)), dma((n,)), dma((2 * steps * n,)), dma((2 * steps * n,))]

    def local(self, m):
        return pltpu.make_async_copy(self.terms[m].at[:, self.p.c], self.own[m], self.own_sem.at[m])

    def pair(self, m):
        return remote(self.terms[m].at[:, 1 - self.p.c], self.other[m], self.pair_send.at[m], self.pair_recv.at[m], self.p.sibling)

    def goes(self, direction, step, m):
        return step > 0 or self.signs[m] == direction

    def slot(self, direction, step):
        return (direction < 0) * self.p.half + step

    def ring(self, direction, step, m):
        slot = self.slot(direction, step)
        k = slot * len(self.terms) + m
        return remote(self.sent[m].at[slot], self.came[m].at[slot], self.ring_send.at[k], self.ring_recv.at[k], self.p.beside(direction))

    def exchange(self):
        for m in range(len(self.terms)):
            self.pair(m).start()
            self.local(m).start()

    def mine(self, m, t):
        return self.own[m][t].astype(F32) + self.other[m][t].astype(F32)

    def step(self, step):
        for m in range(len(self.terms)):
            if step == 0:
                self.local(m).wait()
                self.pair(m).wait_recv()
            for direction in DIRECTIONS:
                if not self.goes(direction, step, m):
                    continue
                value = self.mine(m, self.p.chip(direction * (self.p.half - step)))
                if step > 0 and self.goes(direction, step - 1, m):
                    self.ring(direction, step - 1, m).wait_recv()
                    value = value + self.came[m][self.slot(direction, step - 1)].astype(F32)
                self.sent[m][self.slot(direction, step)] = value.astype(BF16)
                self.ring(direction, step, m).start()

    def result(self, m):
        last = self.p.half - 1
        value = self.mine(m, self.p.z)
        for direction in DIRECTIONS:
            self.ring(direction, last, m).wait_recv()
            value = value + self.came[m][self.slot(direction, last)].astype(F32)
        return value.astype(BF16)

    def finish(self):
        for m in range(len(self.terms)):
            self.pair(m).wait_send()
            for direction in DIRECTIONS:
                for step in range(self.p.half):
                    if self.goes(direction, step, m):
                        self.ring(direction, step, m).wait_send()


GATHER_SIGNS = (1, -1, 1)


def gather_kernel(chips, *refs):
    shards, fulls, sems = refs[:3], refs[3:6], refs[6:]
    place = Place(chips)
    meet([place.sibling, place.beside(1), place.beside(-1)])
    gather = Gather(place, shards, fulls, GATHER_SIGNS, *sems)
    for step in range(place.half + 1):
        gather.step(step)
    gather.finish()


def forward_kernel(chips, x, wg, wu, wd, s0, s1, s2, h_out, act_out, f0, f1, f2, *sems):
    i, n = pl.program_id(0), pl.num_programs(0)
    place = Place(chips)
    gather = Gather(place, (s0, s1, s2), (f0, f1, f2), GATHER_SIGNS, *sems)
    for step in range(place.half + 1):

        @pl.when(i == (3 * step) // 2)
        def _(step=step):
            if step == 0:
                meet([place.sibling, place.beside(1), place.beside(-1)])
            gather.step(step)

    h = x[...]
    _, _, a = norm_parts(h)
    gate, up = dot(a, wg[...]), dot(a, wu[...])
    act = (gate * sigmoid(gate) * up).astype(BF16)
    act_out[...] = act
    out = dot(act, wd[...]).astype(BF16)
    h_out[...] = (h.astype(F32) + out.astype(F32)).astype(BF16)

    @pl.when(i == n - 1)
    def _():
        gather.finish()


def backward_act(a, by_out, wg, wu, wdt):
    gate, up = dot(a, wg), dot(a, wu)
    by_act = dot(by_out, wdt).astype(BF16).astype(F32)
    sig = sigmoid(gate)
    silu = gate * sig
    act = (silu * up).astype(BF16)
    by_up = (by_act * silu).astype(BF16)
    by_gate = (by_act * up * (sig + silu * (1.0 - sig))).astype(BF16)
    return act, by_gate, by_up


def both_kernel(h, dy, act0, wg, wu, wd, dh_out, gg, gu, gd, gd0, wgt, wut, wdt, ag, au, ad, ad0):
    i, n = pl.program_id(0), pl.num_programs(0)

    @pl.when(i == 0)
    def _():
        wgt[...] = wg[...].T
        wut[...] = wu[...].T
        wdt[...] = wd[...].T
        for acc in (ag, au, ad, ad0):
            acc[...] = jnp.zeros_like(acc)

    by_out = dy[...]
    wide, scale, a = norm_parts(h[...])
    act, by_gate, by_up = backward_act(a, by_out, wg[...], wu[...], wdt[...])
    at = a.T
    ag[...] += dot(at, by_gate)
    au[...] += dot(at, by_up)
    ad[...] += dot(by_out.T, act)
    by_a = dot(by_gate, wgt[...]).astype(BF16).astype(F32) + dot(by_up, wut[...]).astype(BF16).astype(F32)
    by_a = by_a.astype(BF16).astype(F32)
    by_wide = by_a * scale - wide * (scale * scale * scale * jnp.mean(by_a * wide, -1, keepdims=True))
    by_h = (by_out.astype(F32) + by_wide.astype(BF16).astype(F32)).astype(BF16)
    dh_out[...] = by_h
    ad0[...] += dot(by_h.T, act0[...])

    @pl.when(i == n - 1)
    def _():
        gg[...] = ag[...].astype(BF16)
        gu[...] = au[...].astype(BF16)
        gd[...] = ad[...].astype(BF16).T
        gd0[...] = ad0[...].astype(BF16).T


def backward_kernel(chips, x, dh, wg, wu, wd, t0, t1, t2, t3, gg, gu, r0, r1, r2, r3, wdt, ag, au, *scratch):
    i, n = pl.program_id(0), pl.num_programs(0)
    place = Place(chips)
    scatter = Scatter(place, (t0, t1, t2, t3), (1, -1, 1, -1), scratch)

    @pl.when(i == 0)
    def _():
        meet([place.sibling, place.beside(1), place.beside(-1)])
        scatter.exchange()
        wdt[...] = wd[...].T
        ag[...] = jnp.zeros_like(ag)
        au[...] = jnp.zeros_like(au)

    for step in range(place.half):

        @pl.when(i == step + 1)
        def _(step=step):
            scatter.step(step)

    _, _, a = norm_parts(x[...])
    _, by_gate, by_up = backward_act(a, dh[...], wg[...], wu[...], wdt[...])
    at = a.T
    ag[...] += dot(at, by_gate)
    au[...] += dot(at, by_up)

    @pl.when(i == n - 1)
    def _():
        for m, out in enumerate((r0, r1, r2, r3)):
            out[...] = scatter.result(m)
        scatter.finish()
        gg[...] = ag[...].astype(BF16)
        gu[...] = au[...].astype(BF16)


def last_kernel(chips, t0, t1, g0, g1, g2, g3, r0, r1, total, part, parts, part_send, part_recv, *scratch):
    place = Place(chips)
    n = 2 * chips
    me = lax.axis_index("dp")
    scatter = Scatter(place, (t0, t1), (1, -1), scratch)
    meet([lax.rem(me + k, n) for k in range(1, n)])
    scatter.exchange()
    squares = jnp.zeros((8, 128), F32)

    def add_up(squares, g):
        g = g.astype(F32)
        g = (g * g).reshape(g.shape[0] // 8, 8, g.shape[1]).sum(0)
        return squares + sum(g[:, k : k + 128] for k in range(0, g.shape[1], 128))

    for g in (g0, g1, g2, g3):
        squares = add_up(squares, g[...])
    for step in range(place.half):
        scatter.step(step)
    for m, out in enumerate((r0, r1)):
        value = scatter.result(m)
        out[...] = value
        squares = add_up(squares, value)
    part[...] = squares
    copies = [remote(part, parts.at[n - k - 1], part_send.at[k - 1], part_recv.at[n - k - 1], lax.rem(me + k, n)) for k in range(1, n)]
    for copy in copies:
        copy.start()
    total_squares = squares
    for k in range(1, n):
        remote(part, parts.at[k - 1], part_send.at[k - 1], part_recv.at[k - 1], lax.rem(me + k, n)).wait_recv()
        total_squares = total_squares + parts[k - 1]
    for copy in copies:
        copy.wait_send()
    scatter.finish()
    total[...] = total_squares


def whole(shape=None):
    return pl.BlockSpec(memory_space=pltpu.VMEM) if shape is None else pl.BlockSpec(shape, lambda i: (0,) * len(shape), pipeline_mode=pl.Buffered(1))


def params(collective=None, **more):
    if collective is not None:
        more.update(collective_id=collective, has_side_effects=True)
    return pltpu.CompilerParams(vmem_limit_bytes=VMEM_LIMIT, **more)


def adamw(w, m, v, g):
    m = 0.9 * m + 0.1 * g
    v = 0.95 * v + 0.05 * g * g
    step = m * lax.rsqrt(v + 1e-8) + 0.1 * w
    return (w - 0.02 * step).astype(BF16), m, v


def solution(mesh):
    group = mesh.shape["dp"]
    chips = group // 2
    any_space = pl.BlockSpec(memory_space=pl.ANY)

    def step(x, dy, *arrays):
        weights, ms, vs = (arrays[i : i + 3] for i in (0, 3, 6))
        x, dy = x[0], dy[0]
        tokens, d = x.shape
        tiles = tokens // TILE
        rows = [(w.shape[1], w.shape[2]) for w in weights]
        ff = rows[0][1]
        shards = [[w[layer] for w in weights] for layer in range(2)]
        full_types = [jax.ShapeDtypeStruct((chips, 2, *r), BF16) for r in rows]
        joined = [(group * r[0], r[1]) for r in rows]

        def join(fulls):
            return [f.reshape(j) for f, j in zip(fulls, joined)]

        def split(g, m):
            return g.reshape(chips, 2, *rows[m])

        w0 = pl.pallas_call(
            functools.partial(gather_kernel, chips),
            out_shape=full_types,
            in_specs=[whole()] * 3,
            out_specs=[whole()] * 3,
            scratch_shapes=Gather.scratch(chips, 3),
            compiler_params=params(0),
            name="gather0",
        )(*shards[0])
        w0 = join(w0)

        narrow = pl.BlockSpec((TILE, d), lambda i: (i, 0))
        broad = pl.BlockSpec((TILE, ff), lambda i: (i, 0))
        weight_specs = [whole(j) for j in joined]
        tokens_d = jax.ShapeDtypeStruct((tokens, d), BF16)
        tokens_ff = jax.ShapeDtypeStruct((tokens, ff), BF16)
        h1, act0, *w1 = pl.pallas_call(
            functools.partial(forward_kernel, chips),
            grid=(tiles,),
            out_shape=[tokens_d, tokens_ff, *full_types],
            in_specs=[narrow, *weight_specs, *[whole(r) for r in rows]],
            out_specs=[narrow, broad, *[any_space] * 3],
            scratch_shapes=Gather.scratch(chips, 3),
            compiler_params=params(1, dimension_semantics=("arbitrary",)),
            name="forward0",
        )(x, *w0, *shards[1])
        w1 = join(w1)

        wide = jax.ShapeDtypeStruct((d, ff), BF16)
        tall = jax.ShapeDtypeStruct((ff, d), BF16)
        dh, gg1, gu1, gd1, gd0 = pl.pallas_call(
            both_kernel,
            grid=(tiles,),
            out_shape=[tokens_d, wide, wide, tall, tall],
            in_specs=[narrow, narrow, broad, *weight_specs],
            out_specs=[narrow, whole((d, ff)), whole((d, ff)), whole((ff, d)), whole((ff, d))],
            scratch_shapes=[pltpu.VMEM((ff, d), BF16), pltpu.VMEM((ff, d), BF16), pltpu.VMEM((d, ff), BF16)] + [pltpu.VMEM((d, ff), F32)] * 4,
            compiler_params=params(dimension_semantics=("arbitrary",)),
            name="both1",
        )(h1, dy, act0, *w1)

        blocks = [jax.ShapeDtypeStruct(r, BF16) for r in rows]
        gg0, gu0, rg1, ru1, rd1, rd0 = pl.pallas_call(
            functools.partial(backward_kernel, chips),
            grid=(tiles,),
            out_shape=[wide, wide, *blocks, blocks[2]],
            in_specs=[narrow, narrow, *weight_specs, *[any_space] * 4],
            out_specs=[whole((d, ff)), whole((d, ff)), *[whole(r) for r in rows], whole(rows[2])],
            scratch_shapes=[pltpu.VMEM((d, ff), BF16)] + [pltpu.VMEM((d, ff), F32)] * 2 + Scatter.scratch(chips, [*rows, rows[2]]),
            compiler_params=params(2, dimension_semantics=("arbitrary",)),
            name="backward0",
        )(x, dh, *w0, split(gg1, 0), split(gu1, 1), split(gd1, 2), split(gd0, 2))

        rg0, ru0, total = pl.pallas_call(
            functools.partial(last_kernel, chips),
            out_shape=[blocks[0], blocks[1], jax.ShapeDtypeStruct((8, 128), F32)],
            in_specs=[any_space] * 2 + [whole()] * 4,
            out_specs=[whole()] * 3,
            scratch_shapes=[pltpu.VMEM((8, 128), F32), pltpu.VMEM((group - 1, 8, 128), F32)]
            + [pltpu.SemaphoreType.DMA((group - 1,))] * 2
            + Scatter.scratch(chips, rows[:2]),
            compiler_params=params(3),
            name="scatter0",
        )(split(gg0, 0), split(gu0, 1), rg1, ru1, rd1, rd0)

        count = group * sum(w.size for w in weights)
        factor = jnp.minimum(1.0, 0.5 * lax.rsqrt(jnp.sum(total) / count + 1e-30))
        gradients = [jnp.stack(pair).astype(F32) * factor for pair in ((rg0, rg1), (ru0, ru1), (rd0, rd1))]
        new = [adamw(w.astype(F32), m, v, g) for w, m, v, g in zip(weights, ms, vs, gradients, strict=True)]
        return tuple(one[which] for which in range(3) for one in new)

    states, cut = P(("rep", "dp"), None, None), P(None, "dp", None)
    return jax.shard_map(
        step,
        mesh=mesh,
        in_specs=(states, states) + (cut,) * 9,
        out_specs=(P("rep", "dp", None),) * 9,
        check_vma=False,
    )
```

```python
import functools
import math

import jax
import jax.numpy as jnp
from jax import lax
from jax.experimental import pallas as pl
from jax.experimental.pallas import tpu as pltpu
from jax.sharding import PartitionSpec as P

F32, BF16 = jnp.float32, jnp.bfloat16
TILE = 512
VMEM_LIMIT = 60 << 20
MESH = pl.DeviceIdType.MESH


def dot(a, b):
    return jnp.dot(a, b, preferred_element_type=F32)


def norm_parts(h):
    wide = h.astype(F32)
    scale = lax.rsqrt(jnp.mean(wide * wide, -1, keepdims=True) + 1e-6)
    return wide, scale, (wide * scale).astype(BF16)


def sigmoid(x):
    return 0.5 * jnp.tanh(0.5 * x) + 0.5


class Place:
    def __init__(self, chips, groups=None):
        self.dp = me = lax.axis_index("dp")
        if groups is not None:
            rep, length = lax.axis_index("rep"), math.isqrt(groups)
            x, y = rep // length, rep % length
            self.parity = (x + y) % 2
            self.across = ((x + 1 - 2 * (x % 2)) * length + y, x * length + y + 1 - 2 * (y % 2))
        self.chips, self.half = chips, chips // 2
        self.z, self.c = me // 2, me % 2
        self.sibling = self.z * 2 + 1 - self.c

    def chip(self, offset):
        return lax.rem(self.z + offset + 2 * self.chips, self.chips)

    def beside(self, direction):
        return self.chip(direction) * 2 + self.c


def ident(device, group=None):
    return {"dp": device} if group is None else {"rep": group, "dp": device}


def meet(devices):
    barrier = pltpu.get_barrier_semaphore()
    for device in devices:
        pl.semaphore_signal(barrier, inc=1, device_id=ident(*device), device_id_type=MESH)
    pl.semaphore_wait(barrier, len(devices))


def remote(src, dst, send, recv, device, group=None):
    return pltpu.make_async_remote_copy(src_ref=src, dst_ref=dst, send_sem=send, recv_sem=recv, device_id=ident(device, group), device_id_type=MESH)


DIRECTIONS = (1, -1)


class Gather:
    PIECES = 4
    SIGNS = (1, -1, 1, -1)

    def __init__(self, place, layer, shards, gu, down, sems):
        self.p, self.shards, self.gu, self.down = place, [s.at[layer] for s in shards], gu, down
        self.ring_send, self.ring_recv, self.cross_send, self.cross_recv, self.side_send, self.side_recv, self.own_sem = sems
        self.rows, self.ff = self.shards[0].shape
        self.d = self.shards[2].shape[1]

    @staticmethod
    def scratch(chips):
        ring, dma = 2 * (chips // 2) * Gather.PIECES, pltpu.SemaphoreType.DMA
        return [dma((ring,)), dma((ring,)), dma((Gather.PIECES,)), dma((ring,)), dma((2,)), dma((2,)), dma((3,))]

    def goes(self, direction, step, m):
        return step < self.p.half - 1 or self.SIGNS[m] == direction

    def part(self, m, parity):
        if m < 2:
            half = self.rows // 2
            return pl.ds(pl.multiple_of(parity * half, half), half), slice(None)
        quarter = self.d // 4
        return slice(None), pl.ds(pl.multiple_of((2 * parity + m - 2) * quarter, quarter), quarter)

    def block(self, m, chip, core):
        return self.down.at[chip, core] if m >= 2 else self.gu.at[chip, core, :, m * self.ff : (m + 1) * self.ff]

    def piece(self, m, chip, parity):
        return self.block(m, chip, self.p.c).at[self.part(m, parity)]

    def source(self, direction, step, m, parity):
        if step == 0:
            return self.shards[min(m, 2)].at[self.part(m, parity)]
        return self.piece(m, self.p.chip(-direction * step), parity)

    def index(self, direction, step, m):
        return ((direction < 0) * self.p.half + step) * self.PIECES + m

    def ring(self, direction, step, m):
        p, k = self.p, self.index(direction, step, m)
        place = self.piece(m, p.chip(-direction * step), p.parity)
        return remote(self.source(direction, step, m, p.parity), place, self.ring_send.at[k], self.ring_recv.at[k], p.beside(direction))

    def cross(self, direction, step, m):
        p, k = self.p, self.index(direction, step, m)
        place = self.piece(m, p.chip(-direction * (step + 1)), p.parity)
        return remote(place, place, self.cross_send.at[m], self.cross_recv.at[k], p.dp, p.across[m % 2])

    def side(self, ref, m):
        return remote(ref, ref, self.side_send.at[m // 2], self.side_recv.at[m // 2], self.p.sibling)

    def own(self, m):
        return pltpu.make_async_copy(self.shards[m], self.block(m, self.p.z, self.p.c), self.own_sem.at[m])

    def start(self):
        p = self.p
        for m in range(self.PIECES):
            for direction in DIRECTIONS:
                if self.goes(direction, 0, m):
                    self.ring(direction, 0, m).start()
        for m in range(3):
            self.own(m).start()
            place = self.block(m, p.z, p.c)
            remote(self.shards[m], place, self.side_send.at[m // 2], self.side_recv.at[m // 2], p.sibling).start()

    def step(self, step, m):
        p = self.p
        for direction in DIRECTIONS:
            if self.goes(direction, step - 1, m):
                self.ring(direction, step - 1, m).wait_recv()
                if step < p.half and self.goes(direction, step, m):
                    self.ring(direction, step, m).start()
                self.cross(direction, step - 1, m).start()
                self.side(self.piece(m, p.chip(-direction * step), p.parity), m).start()

    def crossed(self, step, m):
        p = self.p
        for direction in DIRECTIONS:
            if self.goes(direction, step - 1, m):
                chip = p.chip(-direction * step)
                k = self.index(direction, step - 1, m)
                place = self.piece(m, chip, 1 - p.parity)
                remote(place, place, self.cross_send.at[m], self.cross_recv.at[k], p.dp, p.across[m % 2]).wait_recv()
                self.side(place, m).start()

    def finish(self):
        p = self.p
        for m in range(3):
            self.own(m).wait()
        for m, ref in ((0, self.gu), (2, self.down)):
            self.side(ref.at[:, 0], m).wait()
        for m in range(self.PIECES):
            sent = self.block(m, slice(0, p.chips - 1), 0).at[(slice(None), *self.first(m))]
            remote(sent, sent, self.cross_send.at[m], self.cross_recv.at[0], p.dp, p.across[m % 2]).wait_send()
            for direction in DIRECTIONS:
                for step in range(p.half):
                    if self.goes(direction, step, m):
                        self.ring(direction, step, m).wait_send()

    def first(self, m):
        return (slice(0, self.rows // 2), slice(None)) if m < 2 else (slice(None), slice(0, self.d // 4))


class Scatter:
    def __init__(self, place, terms, signs, scratch, in_hbm):
        self.p, self.terms, self.signs, self.in_hbm, n = place, terms, signs, in_hbm, len(terms)
        scratch = list(scratch)
        take = lambda k: [scratch.pop(0) for _ in range(k)]
        self.other, self.sent, self.came = take(n), take(n), take(n)
        self.own = take(n) if in_hbm else None
        self.pair_send, self.pair_recv, self.ring_send, self.ring_recv, self.own_sem = scratch

    @staticmethod
    def scratch(chips, shapes, in_hbm):
        steps, n, dma = chips // 2, len(shapes), pltpu.SemaphoreType.DMA
        blocks = [pltpu.VMEM((chips, *shape), BF16) for shape in shapes]
        slots = [pltpu.VMEM((2 * steps, *shape), BF16) for shape in shapes]
        return blocks + slots * 2 + blocks * in_hbm + [dma((n,)), dma((n,)), dma((2 * steps * n,)), dma((2 * steps * n,)), dma((n,))]

    def local(self, m):
        return pltpu.make_async_copy(self.terms[m].at[:, self.p.c], self.own[m], self.own_sem.at[m])

    def pair(self, m):
        return remote(self.terms[m].at[:, 1 - self.p.c], self.other[m], self.pair_send.at[m], self.pair_recv.at[m], self.p.sibling)

    def goes(self, direction, step, m):
        return step > 0 or self.signs[m] == direction

    def slot(self, direction, step):
        return (direction < 0) * self.p.half + step

    def ring(self, direction, step, m):
        slot = self.slot(direction, step)
        k = slot * len(self.terms) + m
        return remote(self.sent[m].at[slot], self.came[m].at[slot], self.ring_send.at[k], self.ring_recv.at[k], self.p.beside(direction))

    def exchange(self):
        for m in range(len(self.terms)):
            self.pair(m).start()
            if self.in_hbm:
                self.local(m).start()

    def mine(self, m, t):
        own = self.own[m][t] if self.in_hbm else self.terms[m][t, self.p.c]
        return own.astype(F32) + self.other[m][t].astype(F32)

    def step(self, step):
        for m in range(len(self.terms)):
            if step == 0:
                if self.in_hbm:
                    self.local(m).wait()
                self.pair(m).wait_recv()
            for direction in DIRECTIONS:
                if not self.goes(direction, step, m):
                    continue
                value = self.mine(m, self.p.chip(direction * (self.p.half - step)))
                if step > 0 and self.goes(direction, step - 1, m):
                    self.ring(direction, step - 1, m).wait_recv()
                    value = value + self.came[m][self.slot(direction, step - 1)].astype(F32)
                self.sent[m][self.slot(direction, step)] = value.astype(BF16)
                self.ring(direction, step, m).start()

    def result(self, m):
        last = self.p.half - 1
        value = self.mine(m, self.p.z)
        for direction in DIRECTIONS:
            self.ring(direction, last, m).wait_recv()
            value = value + self.came[m][self.slot(direction, last)].astype(F32)
        return value.astype(BF16)

    def finish(self):
        for m in range(len(self.terms)):
            self.pair(m).wait_send()
            for direction in DIRECTIONS:
                for step in range(self.p.half):
                    if self.goes(direction, step, m):
                        self.ring(direction, step, m).wait_send()


CHUNKS = (512, 512, 384)
SCHEDULE = {
    "first": (2, 3, 5, 7, 10),
    "second": (2, 4, 6, 8, 11),
    "chunk0": (4, 5, 6, 8, 10),
    "chunk1": (8, 9, 11),
}


def forward_kernel(chips, groups, x, s0, s1, s2, h_out, act_out, a_out, at_out, w0gu, w0d, w1gu, w1d, gu, down, keep_sem, *sems):
    i, n = pl.program_id(0), pl.num_programs(0)
    place = Place(chips, groups)
    ff = s0.shape[2]
    d = x.shape[1]
    half = len(sems) // 2
    one = Gather(place, 0, (s0, s1, s2), gu, down, sems[:half])
    two = Gather(place, 1, (s0, s1, s2), w1gu, w1d, sems[half:])
    keep = [pltpu.make_async_copy(src, dst, keep_sem.at[k]) for k, (src, dst) in enumerate(((gu, w0gu), (down, w0d)))]
    last = place.half
    pieces = range(Gather.PIECES)

    @pl.when(i == 0)
    def _():
        meet([(place.sibling,), (place.beside(1),), (place.beside(-1),), *[(place.dp, group) for group in place.across]])
        one.start()
        for step in range(1, last + 1):
            for m in pieces:
                one.step(step, m)
                if step > 1:
                    one.crossed(step - 1, m)
        two.start()
        for m in pieces:
            one.crossed(last, m)
        one.finish()
        for copy in keep:
            copy.start()

    for step in range(1, last + 1):

        @pl.when(i == step)
        def _(step=step):
            for m in pieces:
                two.step(step, m)
                if step > 1:
                    two.crossed(step - 1, m)

    @pl.when(i == last + 1)
    def _():
        for m in pieces:
            two.crossed(last, m)

    h = x[...]
    _, _, a = norm_parts(h)
    a_out[...] = a
    at_out[...] = a.T
    both = dot(a, gu[...].reshape(d, 2 * ff))
    gate, up = both[:, :ff], both[:, ff:]
    act = (gate * sigmoid(gate) * up).astype(BF16)
    act_out[...] = act
    out = dot(act, down[...].reshape(ff, d)).astype(BF16)
    h_out[...] = (h.astype(F32) + out.astype(F32)).astype(BF16)

    @pl.when(i == n - 1)
    def _():
        two.finish()
        for copy in keep:
            copy.wait()


def act_backward(gate, up, by_act):
    by_act = by_act.astype(BF16).astype(F32)
    sig = sigmoid(gate)
    silu = gate * sig
    act = (silu * up).astype(BF16)
    by_up = (by_act * silu).astype(BF16)
    by_gate = (by_act * up * (sig + silu * (1.0 - sig))).astype(BF16)
    return act, by_gate, by_up


def both_kernel(h, dy, act0, wgu, wd, dh_out, gg, gu, gd, gd0, wgut, wdt, by_gu, agu, ad, ad0):
    i, n = pl.program_id(0), pl.num_programs(0)
    ff = wd.shape[0]

    @pl.when(i == 0)
    def _():
        wgut[...] = wgu[...].T
        wdt[...] = wd[...].T
        for acc in (agu, ad, ad0):
            acc[...] = jnp.zeros_like(acc)

    by_out = dy[...]
    wide, scale, a = norm_parts(h[...])
    both = dot(a, wgu[...])
    act, by_gate, by_up = act_backward(both[:, :ff], both[:, ff:], dot(by_out, wdt[...]))
    by_gu[:, :ff] = by_gate
    by_gu[:, ff:] = by_up
    by_a = dot(by_gu[...], wgut[...]).astype(BF16).astype(F32)
    agu[...] += dot(a.T, by_gu[...])
    ad[...] += dot(by_out.T, act)
    by_wide = by_a * scale - wide * (scale * scale * scale * jnp.mean(by_a * wide, -1, keepdims=True))
    by_h = (by_out.astype(F32) + by_wide.astype(BF16).astype(F32)).astype(BF16)
    dh_out[...] = by_h
    ad0[...] += dot(by_h.T, act0[...])

    @pl.when(i == n - 1)
    def _():
        gg[...] = agu[:, :ff].astype(BF16)
        gu[...] = agu[:, ff:].astype(BF16)
        gd[...] = ad[...].astype(BF16).T
        gd0[...] = ad0[...].astype(BF16).T


def add_up(squares, g):
    g = g.astype(F32)
    g = (g * g).reshape(g.shape[0] // 8, 8, g.shape[1]).sum(0)
    return squares + sum(g[:, k : k + 128] for k in range(0, g.shape[1], 128))


def backward_kernel(chips, tiles, sizes, a, at, dh, wgu, wd, t0, t1, t2, t3, rg, ru, rg1, ru1, rd1, rd0, total, wdt, ag, au, squares, part, parts, part_send, part_recv, *scratch):
    i = pl.program_id(0)
    place = Place(chips)
    group = 2 * chips
    me = lax.axis_index("dp")
    ff = wd.shape[0]
    scratch = list(scratch)
    take = lambda k: [scratch.pop(0) for _ in range(k)]
    hbm_count, chunk_count = 4 * 2 + 5, 3 * 2 + 5
    first = Scatter(place, (t0, t1), (1, -1), take(hbm_count), True)
    second = Scatter(place, (t2, t3), (1, -1), take(hbm_count), True)
    chunks = []
    for _ in sizes:
        terms = take(2)
        chunks.append(Scatter(place, terms, (1, -1), take(chunk_count), False))
    steps = place.half
    starts = [sum(sizes[:k]) for k in range(len(sizes))]

    def settle(scatter, outs):
        sums = squares[...]
        for m, out in enumerate(outs):
            value = scatter.result(m)
            out[...] = value
            sums = add_up(sums, value)
        squares[...] = sums
        scatter.finish()

    def chunk_outs(k):
        return [r.at[:, starts[k] : starts[k] + sizes[k]] for r in (rg, ru)]

    events = []
    for name, scatter, outs in (("first", first, (rg1, ru1)), ("second", second, (rd1, rd0))):
        times = SCHEDULE[name]
        events += [(times[s], functools.partial(scatter.step, s)) for s in range(steps)]
        events.append((times[steps], functools.partial(settle, scatter, outs)))
    for k in range(len(sizes) - 1):
        times = SCHEDULE[f"chunk{k}"]
        for s in range(len(times) - 1):
            events.append((times[s + 1], functools.partial(chunks[k].step, s) if s < steps else functools.partial(settle, chunks[k], chunk_outs(k))))

    def clear():
        ag[...] = jnp.zeros_like(ag)
        au[...] = jnp.zeros_like(au)

    @pl.when(i == 0)
    def _():
        others = [lax.rem(me + k, group) for k in range(1, group)]
        meet([(other,) for other in others])
        first.exchange()
        second.exchange()
        squares[...] = jnp.zeros_like(squares)
        wdt[...] = wd[...].T
        clear()

    for when in sorted({when for when, _ in events}):

        @pl.when(i == when)
        def _(now=when):
            for when, act in events:
                if when == now:
                    act()

    for k, size in enumerate(sizes):

        @pl.when(i // tiles == k)
        def _(k=k, size=size):
            cols = slice(starts[k], starts[k] + size)
            by_out = dh[...]
            gate, up = dot(a[...], wgu[:, cols]), dot(a[...], wgu[:, ff + cols.start : ff + cols.stop])
            _, by_gate, by_up = act_backward(gate, up, dot(by_out, wdt[:, cols]))
            ag[:, :size] += dot(at[...], by_gate)
            au[:, :size] += dot(at[...], by_up)

        @pl.when(i == (k + 1) * tiles - 1)
        def _(k=k, size=size):
            for term, acc in zip(chunks[k].terms, (ag, au)):
                term[...] = acc[:, :size].astype(BF16).reshape(term.shape)
            chunks[k].exchange()
            clear()

    @pl.when(i == len(sizes) * tiles - 1)
    def _():
        done = [len(SCHEDULE[f"chunk{k}"]) - 1 for k in range(len(sizes) - 1)] + [0]
        for s in range(steps):
            for k, chunk in enumerate(chunks):
                if done[k] <= steps and done[k] + s < steps:
                    chunk.step(done[k] + s)
                elif done[k] <= steps and done[k] + s == steps:
                    settle(chunk, chunk_outs(k))
        settle(chunks[-1], chunk_outs(len(sizes) - 1))
        part[...] = squares[...]
        copies = [remote(part, parts.at[group - k - 1], part_send.at[k - 1], part_recv.at[group - k - 1], lax.rem(me + k, group)) for k in range(1, group)]
        for copy in copies:
            copy.start()
        sums = squares[...]
        for k in range(1, group):
            remote(part, parts.at[k - 1], part_send.at[k - 1], part_recv.at[k - 1], lax.rem(me + k, group)).wait_recv()
            sums = sums + parts[k - 1]
        for copy in copies:
            copy.wait_send()
        total[...] = sums


def step_kernel(count, total, *refs):
    ws, ms, vs, gs, outs = refs[:3], refs[3:6], refs[6:9], refs[9:15], refs[15:]
    squares = jnp.sum(jnp.sum(total[...], 0, keepdims=True), 1, keepdims=True)
    factor = jnp.minimum(1.0, 0.5 * lax.rsqrt(squares / count + 1e-30))
    for k in range(3):
        for layer in range(2):
            g = gs[2 * k + layer][...].astype(F32) * factor
            w, m, v = adamw(ws[k][layer].astype(F32), ms[k][layer], vs[k][layer], g)
            outs[k][layer], outs[3 + k][layer], outs[6 + k][layer] = w, m, v


def whole(shape=None):
    return pl.BlockSpec(memory_space=pltpu.VMEM) if shape is None else pl.BlockSpec(shape, lambda i: (0,) * len(shape), pipeline_mode=pl.Buffered(1))


def params(collective=None, **more):
    if collective is not None:
        more.update(collective_id=collective, has_side_effects=True)
    return pltpu.CompilerParams(vmem_limit_bytes=VMEM_LIMIT, **more)


def adamw(w, m, v, g):
    m = 0.9 * m + 0.1 * g
    v = 0.95 * v + 0.05 * g * g
    step = m * lax.rsqrt(v + 1e-8) + 0.1 * w
    return (w - 0.02 * step).astype(BF16), m, v


def solution(mesh):
    group, groups = mesh.shape["dp"], mesh.shape["rep"]
    chips = group // 2
    any_space = pl.BlockSpec(memory_space=pl.ANY)

    def step(x, dy, *arrays):
        weights, ms, vs = (arrays[i : i + 3] for i in (0, 3, 6))
        x, dy = x[0], dy[0]
        tokens, d = x.shape
        tiles = tokens // TILE
        rows = [(w.shape[1], w.shape[2]) for w in weights]
        ff = rows[0][1]
        d_ff = (d, ff)
        gu_blocks = jax.ShapeDtypeStruct((chips, 2, rows[0][0], 2 * ff), BF16)
        down_blocks = jax.ShapeDtypeStruct((chips, 2, *rows[2]), BF16)

        def split(g, m):
            return g.reshape(chips, 2, *rows[m])

        narrow = pl.BlockSpec((TILE, d), lambda i: (i, 0))
        broad = pl.BlockSpec((TILE, ff), lambda i: (i, 0))
        weight_specs = [whole((d, 2 * ff)), whole((ff, d))]
        tokens_d = jax.ShapeDtypeStruct((tokens, d), BF16)
        tokens_ff = jax.ShapeDtypeStruct((tokens, ff), BF16)
        dma = pltpu.SemaphoreType.DMA
        h1, act0, a0, a0t, *full = pl.pallas_call(
            functools.partial(forward_kernel, chips, groups),
            grid=(tiles,),
            out_shape=[tokens_d, tokens_ff, tokens_d, jax.ShapeDtypeStruct((d, tokens), BF16), *[gu_blocks, down_blocks] * 2],
            in_specs=[narrow, *[whole(w.shape) for w in weights]],
            out_specs=[narrow, broad, narrow, pl.BlockSpec((d, TILE), lambda i: (0, i)), *[any_space] * 4],
            scratch_shapes=[pltpu.VMEM(gu_blocks.shape, BF16), pltpu.VMEM(down_blocks.shape, BF16), dma((2,))] + Gather.scratch(chips) * 2,
            compiler_params=params(1, dimension_semantics=("arbitrary",)),
            name="forward0",
        )(x, *weights)
        w0, w1 = ([full[k].reshape(d, 2 * ff), full[k + 1].reshape(ff, d)] for k in (0, 2))

        wide = jax.ShapeDtypeStruct(d_ff, BF16)
        tall = jax.ShapeDtypeStruct((ff, d), BF16)
        dh, gg1, gu1, gd1, gd0 = pl.pallas_call(
            both_kernel,
            grid=(tiles,),
            out_shape=[tokens_d, wide, wide, tall, tall],
            in_specs=[narrow, narrow, broad, *weight_specs],
            out_specs=[narrow, whole(d_ff), whole(d_ff), whole((ff, d)), whole((ff, d))],
            scratch_shapes=[pltpu.VMEM((2 * ff, d), BF16), pltpu.VMEM(d_ff, BF16), pltpu.VMEM((TILE, 2 * ff), BF16)]
            + [pltpu.VMEM((d, 2 * ff), F32)]
            + [pltpu.VMEM(d_ff, F32)] * 2,
            compiler_params=params(dimension_semantics=("arbitrary",)),
            name="both1",
        )(h1, dy, act0, *w1)

        blocks = [jax.ShapeDtypeStruct(r, BF16) for r in rows]
        sizes = CHUNKS
        scratch = [pltpu.VMEM(d_ff, BF16)] + [pltpu.VMEM((d, max(sizes)), F32)] * 2
        scratch += [pltpu.VMEM((8, 128), F32)] * 2 + [pltpu.VMEM((group - 1, 8, 128), F32)] + [dma((group - 1,))] * 2
        scratch += Scatter.scratch(chips, rows[:2], True) + Scatter.scratch(chips, [rows[2]] * 2, True)
        for size in sizes:
            block = (rows[0][0], size)
            scratch += [pltpu.VMEM((chips, 2, *block), BF16)] * 2 + Scatter.scratch(chips, [block] * 2, False)
        tiles = tokens // (2 * TILE)
        again = pl.BlockSpec((2 * TILE, d), lambda i: (lax.rem(i, tiles), 0))
        across = pl.BlockSpec((d, 2 * TILE), lambda i: (0, lax.rem(i, tiles)))
        rg0, ru0, rg1, ru1, rd1, rd0, total = pl.pallas_call(
            functools.partial(backward_kernel, chips, tiles, sizes),
            grid=(len(sizes) * tiles,),
            out_shape=[blocks[0], blocks[1], *blocks, blocks[2], jax.ShapeDtypeStruct((8, 128), F32)],
            in_specs=[again, across, again, *weight_specs, *[any_space] * 4],
            out_specs=[whole(r) for r in (rows[0], rows[1], *rows, rows[2], (8, 128))],
            scratch_shapes=scratch,
            compiler_params=params(2, dimension_semantics=("arbitrary",)),
            name="backward0",
        )(a0, a0t, dh, *w0, split(gg1, 0), split(gu1, 1), split(gd1, 2), split(gd0, 2))

        count = group * sum(w.size for w in weights)
        new = [jax.ShapeDtypeStruct(w.shape, t) for t in (BF16, F32, F32) for w in weights]
        return tuple(
            pl.pallas_call(
                functools.partial(step_kernel, count),
                out_shape=new,
                in_specs=[whole()] * 16,
                out_specs=[whole()] * 9,
                compiler_params=params(),
                name="adamw",
            )(total, *weights, *ms, *vs, rg0, rg1, ru0, ru1, rd0, rd1)
        )

    states, cut = P(("rep", "dp"), None, None), P(None, "dp", None)
    return jax.shard_map(
        step,
        mesh=mesh,
        in_specs=(states, states) + (cut,) * 9,
        out_specs=(P("rep", "dp", None),) * 9,
        check_vma=False,
    )
```

```python
import functools
import math

import jax
import jax.numpy as jnp
from jax import lax
from jax.experimental import pallas as pl
from jax.experimental.pallas import tpu as pltpu
from jax.sharding import PartitionSpec as P

F32, BF16 = jnp.float32, jnp.bfloat16
TILE = 512
VMEM_LIMIT = 60 << 20
MESH = pl.DeviceIdType.MESH


def dot(a, b):
    return jnp.dot(a, b, preferred_element_type=F32)


def norm_parts(h):
    wide = h.astype(F32)
    scale = lax.rsqrt(jnp.mean(wide * wide, -1, keepdims=True) + 1e-6)
    return wide, scale, (wide * scale).astype(BF16)


def sigmoid(x):
    return 0.5 * jnp.tanh(0.5 * x) + 0.5


class Place:
    def __init__(self, chips, groups=None):
        self.dp = me = lax.axis_index("dp")
        if groups is not None:
            rep, length = lax.axis_index("rep"), math.isqrt(groups)
            x, y = rep // length, rep % length
            self.parity = (x + y) % 2
            self.across = ((x + 1 - 2 * (x % 2)) * length + y, x * length + y + 1 - 2 * (y % 2))
        self.chips, self.half = chips, chips // 2
        self.z, self.c = me // 2, me % 2
        self.sibling = self.z * 2 + 1 - self.c

    def chip(self, offset):
        return lax.rem(self.z + offset + 2 * self.chips, self.chips)

    def beside(self, direction):
        return self.chip(direction) * 2 + self.c


def ident(device, group=None):
    return {"dp": device} if group is None else {"rep": group, "dp": device}


def meet(devices):
    barrier = pltpu.get_barrier_semaphore()
    for device in devices:
        pl.semaphore_signal(barrier, inc=1, device_id=ident(*device), device_id_type=MESH)
    pl.semaphore_wait(barrier, len(devices))


def remote(src, dst, send, recv, device, group=None):
    return pltpu.make_async_remote_copy(src_ref=src, dst_ref=dst, send_sem=send, recv_sem=recv, device_id=ident(device, group), device_id_type=MESH)


DIRECTIONS = (1, -1)


class Gather:
    PIECES = 4
    SIGNS = (1, -1, 1, -1)

    def __init__(self, place, layer, shards, gu, down, sems):
        self.p, self.shards, self.gu, self.down = place, [s.at[layer] for s in shards], gu, down
        self.ring_send, self.ring_recv, self.cross_send, self.cross_recv, self.side_send, self.side_recv, self.own_sem = sems
        self.rows, self.ff = self.shards[0].shape
        self.d = self.shards[2].shape[1]

    @staticmethod
    def scratch(chips):
        ring, dma = 2 * (chips // 2) * Gather.PIECES, pltpu.SemaphoreType.DMA
        return [dma((ring,)), dma((ring,)), dma((Gather.PIECES,)), dma((ring,)), dma((2,)), dma((2,)), dma((3,))]

    def goes(self, direction, step, m):
        return step < self.p.half - 1 or self.SIGNS[m] == direction

    def part(self, m, parity):
        if m < 2:
            half = self.rows // 2
            return pl.ds(pl.multiple_of(parity * half, half), half), slice(None)
        quarter = self.d // 4
        return slice(None), pl.ds(pl.multiple_of((2 * parity + m - 2) * quarter, quarter), quarter)

    def block(self, m, chip, core):
        return self.down.at[chip, core] if m >= 2 else self.gu.at[chip, core, :, m * self.ff : (m + 1) * self.ff]

    def piece(self, m, chip, parity):
        return self.block(m, chip, self.p.c).at[self.part(m, parity)]

    def source(self, direction, step, m, parity):
        if step == 0:
            return self.shards[min(m, 2)].at[self.part(m, parity)]
        return self.piece(m, self.p.chip(-direction * step), parity)

    def index(self, direction, step, m):
        return ((direction < 0) * self.p.half + step) * self.PIECES + m

    def ring(self, direction, step, m):
        p, k = self.p, self.index(direction, step, m)
        place = self.piece(m, p.chip(-direction * step), p.parity)
        return remote(self.source(direction, step, m, p.parity), place, self.ring_send.at[k], self.ring_recv.at[k], p.beside(direction))

    def cross(self, direction, step, m):
        p, k = self.p, self.index(direction, step, m)
        place = self.piece(m, p.chip(-direction * (step + 1)), p.parity)
        return remote(place, place, self.cross_send.at[m], self.cross_recv.at[k], p.dp, p.across[m % 2])

    def side(self, ref, m):
        return remote(ref, ref, self.side_send.at[m // 2], self.side_recv.at[m // 2], self.p.sibling)

    def own(self, m):
        return pltpu.make_async_copy(self.shards[m], self.block(m, self.p.z, self.p.c), self.own_sem.at[m])

    def start(self):
        p = self.p
        for m in range(self.PIECES):
            for direction in DIRECTIONS:
                if self.goes(direction, 0, m):
                    self.ring(direction, 0, m).start()
        for m in range(3):
            self.own(m).start()
            place = self.block(m, p.z, p.c)
            remote(self.shards[m], place, self.side_send.at[m // 2], self.side_recv.at[m // 2], p.sibling).start()

    def step(self, step, m):
        p = self.p
        for direction in DIRECTIONS:
            if self.goes(direction, step - 1, m):
                self.ring(direction, step - 1, m).wait_recv()
                if step < p.half and self.goes(direction, step, m):
                    self.ring(direction, step, m).start()
                self.cross(direction, step - 1, m).start()
                self.side(self.piece(m, p.chip(-direction * step), p.parity), m).start()

    def crossed(self, step, m):
        p = self.p
        for direction in DIRECTIONS:
            if self.goes(direction, step - 1, m):
                chip = p.chip(-direction * step)
                k = self.index(direction, step - 1, m)
                place = self.piece(m, chip, 1 - p.parity)
                remote(place, place, self.cross_send.at[m], self.cross_recv.at[k], p.dp, p.across[m % 2]).wait_recv()
                self.side(place, m).start()

    def finish(self):
        p = self.p
        for m in range(3):
            self.own(m).wait()
        for m, ref in ((0, self.gu), (2, self.down)):
            self.side(ref.at[:, 0], m).wait()
        for m in range(self.PIECES):
            sent = self.block(m, slice(0, p.chips - 1), 0).at[(slice(None), *self.first(m))]
            remote(sent, sent, self.cross_send.at[m], self.cross_recv.at[0], p.dp, p.across[m % 2]).wait_send()
            for direction in DIRECTIONS:
                for step in range(p.half):
                    if self.goes(direction, step, m):
                        self.ring(direction, step, m).wait_send()

    def first(self, m):
        return (slice(0, self.rows // 2), slice(None)) if m < 2 else (slice(None), slice(0, self.d // 4))


class Scatter:
    def __init__(self, place, terms, signs, scratch, in_hbm):
        self.p, self.terms, self.signs, self.in_hbm, n = place, terms, signs, in_hbm, len(terms)
        scratch = list(scratch)
        take = lambda k: [scratch.pop(0) for _ in range(k)]
        self.other, self.sent, self.came = take(n), take(n), take(n)
        self.own = take(n) if in_hbm else None
        self.pair_send, self.pair_recv, self.ring_send, self.ring_recv, self.own_sem = scratch

    @staticmethod
    def scratch(chips, shapes, in_hbm):
        steps, n, dma = chips // 2, len(shapes), pltpu.SemaphoreType.DMA
        blocks = [pltpu.VMEM((chips, *shape), BF16) for shape in shapes]
        slots = [pltpu.VMEM((2 * steps, *shape), BF16) for shape in shapes]
        return blocks + slots * 2 + blocks * in_hbm + [dma((n,)), dma((n,)), dma((2 * steps * n,)), dma((2 * steps * n,)), dma((n,))]

    def local(self, m):
        return pltpu.make_async_copy(self.terms[m].at[:, self.p.c], self.own[m], self.own_sem.at[m])

    def pair(self, m):
        return remote(self.terms[m].at[:, 1 - self.p.c], self.other[m], self.pair_send.at[m], self.pair_recv.at[m], self.p.sibling)

    def goes(self, direction, step, m):
        return step > 0 or self.signs[m] == direction

    def slot(self, direction, step):
        return (direction < 0) * self.p.half + step

    def ring(self, direction, step, m):
        slot = self.slot(direction, step)
        k = slot * len(self.terms) + m
        return remote(self.sent[m].at[slot], self.came[m].at[slot], self.ring_send.at[k], self.ring_recv.at[k], self.p.beside(direction))

    def exchange(self):
        for m in range(len(self.terms)):
            self.pair(m).start()
            if self.in_hbm:
                self.local(m).start()

    def mine(self, m, t):
        own = self.own[m][t] if self.in_hbm else self.terms[m][t, self.p.c]
        return own.astype(F32) + self.other[m][t].astype(F32)

    def step(self, step):
        for m in range(len(self.terms)):
            if step == 0:
                if self.in_hbm:
                    self.local(m).wait()
                self.pair(m).wait_recv()
            for direction in DIRECTIONS:
                if not self.goes(direction, step, m):
                    continue
                value = self.mine(m, self.p.chip(direction * (self.p.half - step)))
                if step > 0 and self.goes(direction, step - 1, m):
                    self.ring(direction, step - 1, m).wait_recv()
                    value = value + self.came[m][self.slot(direction, step - 1)].astype(F32)
                self.sent[m][self.slot(direction, step)] = value.astype(BF16)
                self.ring(direction, step, m).start()

    def result(self, m):
        last = self.p.half - 1
        value = self.mine(m, self.p.z)
        for direction in DIRECTIONS:
            self.ring(direction, last, m).wait_recv()
            value = value + self.came[m][self.slot(direction, last)].astype(F32)
        return value.astype(BF16)

    def finish(self):
        for m in range(len(self.terms)):
            self.pair(m).wait_send()
            for direction in DIRECTIONS:
                for step in range(self.p.half):
                    if self.goes(direction, step, m):
                        self.ring(direction, step, m).wait_send()


CHUNKS = (512, 512, 384)
SCHEDULE = {
    "first": (2, 4, 6, 8, 10),
    "second": (3, 5, 7, 9, 11),
    "third": (5, 6, 8, 9, 11),
    "run0": (8, 10, 11, 12, 14),
    "run1": (13, 14, 15),
}


def forward_kernel(chips, groups, x, s0, s1, s2, h_out, act_out, a_out, at_out, w0gu, w0d, w1gu, w1d, gu, down, keep_sem, *sems):
    i, n = pl.program_id(0), pl.num_programs(0)
    place = Place(chips, groups)
    ff = s0.shape[2]
    d = x.shape[1]
    half = len(sems) // 2
    one = Gather(place, 0, (s0, s1, s2), gu, down, sems[:half])
    two = Gather(place, 1, (s0, s1, s2), w1gu, w1d, sems[half:])
    keep = [pltpu.make_async_copy(src, dst, keep_sem.at[k]) for k, (src, dst) in enumerate(((gu, w0gu), (down, w0d)))]
    last = place.half
    pieces = range(Gather.PIECES)

    @pl.when(i == 0)
    def _():
        meet([(place.sibling,), (place.beside(1),), (place.beside(-1),), *[(place.dp, group) for group in place.across]])
        one.start()
        for step in range(1, last + 1):
            for m in pieces:
                one.step(step, m)
                if step > 1:
                    one.crossed(step - 1, m)
        two.start()
        for m in pieces:
            one.crossed(last, m)
        one.finish()
        for copy in keep:
            copy.start()

    for step in range(1, last + 1):
        for late, some in enumerate(((0, 1), (2, 3))):

            @pl.when(i == min(2 * step - 1 + late, 2 * last - 1))
            def _(step=step, some=some):
                for m in some:
                    two.step(step, m)
                    if step > 1:
                        two.crossed(step - 1, m)

    h = x[...]
    _, _, a = norm_parts(h)
    a_out[...] = a
    at_out[...] = a.T
    both = dot(a, gu[...].reshape(d, 2 * ff))
    gate, up = both[:, :ff], both[:, ff:]
    act = (gate * sigmoid(gate) * up).astype(BF16)
    act_out[...] = act
    out = dot(act, down[...].reshape(ff, d)).astype(BF16)
    h_out[...] = (h.astype(F32) + out.astype(F32)).astype(BF16)

    @pl.when(i == n - 1)
    def _():
        for m in pieces:
            two.crossed(last, m)
        two.finish()
        for copy in keep:
            copy.wait()


def act_backward(gate, up, by_act):
    by_act = by_act.astype(BF16).astype(F32)
    sig = sigmoid(gate)
    silu = gate * sig
    act = (silu * up).astype(BF16)
    by_up = (by_act * silu).astype(BF16)
    by_gate = (by_act * up * (sig + silu * (1.0 - sig))).astype(BF16)
    return act, by_gate, by_up


def both_kernel(h, dy, wgu, wd, dh_out, dht_out, gg, gu, gd, wgut, wdt, by_gu, agu, ad):
    i, n = pl.program_id(0), pl.num_programs(0)
    ff = wd.shape[0]

    @pl.when(i == 0)
    def _():
        wgut[...] = wgu[...].T
        wdt[...] = wd[...].T
        for acc in (agu, ad):
            acc[...] = jnp.zeros_like(acc)

    by_out = dy[...]
    wide, scale, a = norm_parts(h[...])
    both = dot(a, wgu[...])
    act, by_gate, by_up = act_backward(both[:, :ff], both[:, ff:], dot(by_out, wdt[...]))
    by_gu[:, :ff] = by_gate
    by_gu[:, ff:] = by_up
    by_a = dot(by_gu[...], wgut[...]).astype(BF16).astype(F32)
    agu[...] += dot(a.T, by_gu[...])
    ad[...] += dot(by_out.T, act)
    by_wide = by_a * scale - wide * (scale * scale * scale * jnp.mean(by_a * wide, -1, keepdims=True))
    by_h = (by_out.astype(F32) + by_wide.astype(BF16).astype(F32)).astype(BF16)
    dh_out[...] = by_h
    dht_out[...] = by_h.T

    @pl.when(i == n - 1)
    def _():
        gg[...] = agu[:, :ff].astype(BF16)
        gu[...] = agu[:, ff:].astype(BF16)
        gd[...] = ad[...].astype(BF16).T


def add_up(squares, g):
    g = g.astype(F32)
    g = (g * g).reshape(g.shape[0] // 8, 8, g.shape[1]).sum(0)
    return squares + sum(g[:, k : k + 128] for k in range(0, g.shape[1], 128))


def backward_kernel(chips, tiles, sizes, a, at, dh, dht, act0, wgu, wd, t0, t1, t2, rg, ru, rg1, ru1, rd1, rd0, total, wdt, ad, ag, au, squares, part, parts, part_send, part_recv, *scratch):
    i = pl.program_id(0)
    place = Place(chips)
    group = 2 * chips
    me = lax.axis_index("dp")
    ff = wd.shape[0]
    scratch = list(scratch)
    take = lambda k: [scratch.pop(0) for _ in range(k)]
    first = Scatter(place, (t0, t1), (1, -1), take(4 * 2 + 5), True)
    second = Scatter(place, (t2,), (1,), take(4 + 5), True)
    third = Scatter(place, take(1), (-1,), take(3 + 5), False)
    chunks = []
    for _ in sizes:
        terms = take(2)
        chunks.append(Scatter(place, terms, (1, -1), take(3 * 2 + 5), False))
    steps = place.half
    starts = [sum(sizes[:k]) for k in range(len(sizes))]

    def settle(scatter, outs):
        sums = squares[...]
        for m, out in enumerate(outs):
            value = scatter.result(m)
            out[...] = value
            sums = add_up(sums, value)
        squares[...] = sums
        scatter.finish()

    def chunk_outs(k):
        return [r.at[:, starts[k] : starts[k] + sizes[k]] for r in (rg, ru)]

    events = []
    for name, scatter, outs in (("first", first, (rg1, ru1)), ("second", second, (rd1,)), ("third", third, (rd0,))):
        times = SCHEDULE[name]
        events += [(times[s], functools.partial(scatter.step, s)) for s in range(steps)]
        events.append((times[steps], functools.partial(settle, scatter, outs)))
    for k in range(len(sizes) - 1):
        for s, when in enumerate(SCHEDULE[f"run{k}"]):
            events.append((when, functools.partial(chunks[k].step, s) if s < steps else functools.partial(settle, chunks[k], chunk_outs(k))))

    def clear():
        ag[...] = jnp.zeros_like(ag)
        au[...] = jnp.zeros_like(au)

    @pl.when(i == 0)
    def _():
        others = [lax.rem(me + k, group) for k in range(1, group)]
        meet([(other,) for other in others])
        first.exchange()
        second.exchange()
        squares[...] = jnp.zeros_like(squares)
        wdt[...] = wd[...].T
        clear()
        ad[...] = jnp.zeros_like(ad)

    for when in sorted({when for when, _ in events}):

        @pl.when(i == when)
        def _(now=when):
            for when, act in events:
                if when == now:
                    act()

    @pl.when(i < tiles)
    def _():
        ad[...] += dot(dht[...], act0[...])

    @pl.when(i == tiles - 1)
    def _():
        term = third.terms[0]
        term[...] = ad[...].T.reshape(term.shape).astype(BF16)
        third.exchange()

    for k, size in enumerate(sizes):

        @pl.when(i // tiles == k + 1)
        def _(k=k, size=size):
            cols = slice(starts[k], starts[k] + size)
            by_out = dh[...]
            gate, up = dot(a[...], wgu[:, cols]), dot(a[...], wgu[:, ff + cols.start : ff + cols.stop])
            _, by_gate, by_up = act_backward(gate, up, dot(by_out, wdt[:, cols]))
            ag[:, :size] += dot(at[...], by_gate)
            au[:, :size] += dot(at[...], by_up)

        @pl.when(i == (k + 2) * tiles - 1)
        def _(k=k, size=size):
            for term, acc in zip(chunks[k].terms, (ag, au)):
                term[...] = acc[:, :size].astype(BF16).reshape(term.shape)
            chunks[k].exchange()
            clear()

    @pl.when(i == (len(sizes) + 1) * tiles - 1)
    def _():
        done = [len(SCHEDULE[f"run{k}"]) for k in range(len(sizes) - 1)] + [0]
        for s in range(steps):
            for k, chunk in enumerate(chunks):
                if done[k] <= steps and done[k] + s < steps:
                    chunk.step(done[k] + s)
                elif done[k] <= steps and done[k] + s == steps:
                    settle(chunk, chunk_outs(k))
        settle(chunks[-1], chunk_outs(len(sizes) - 1))
        part[...] = squares[...]
        copies = [remote(part, parts.at[group - k - 1], part_send.at[k - 1], part_recv.at[group - k - 1], lax.rem(me + k, group)) for k in range(1, group)]
        for copy in copies:
            copy.start()
        sums = squares[...]
        for k in range(1, group):
            remote(part, parts.at[k - 1], part_send.at[k - 1], part_recv.at[k - 1], lax.rem(me + k, group)).wait_recv()
            sums = sums + parts[k - 1]
        for copy in copies:
            copy.wait_send()
        total[...] = sums


def step_kernel(count, total, *refs):
    ws, ms, vs, gs, outs = refs[:3], refs[3:6], refs[6:9], refs[9:15], refs[15:]
    squares = jnp.sum(jnp.sum(total[...], 0, keepdims=True), 1, keepdims=True)
    factor = jnp.minimum(1.0, 0.5 * lax.rsqrt(squares / count + 1e-30))
    for k in range(3):
        for layer in range(2):
            g = gs[2 * k + layer][...].astype(F32) * factor
            w, m, v = adamw(ws[k][layer].astype(F32), ms[k][layer], vs[k][layer], g)
            outs[k][layer], outs[3 + k][layer], outs[6 + k][layer] = w, m, v


def whole(shape=None):
    return pl.BlockSpec(memory_space=pltpu.VMEM) if shape is None else pl.BlockSpec(shape, lambda i: (0,) * len(shape), pipeline_mode=pl.Buffered(1))


def params(collective=None, **more):
    if collective is not None:
        more.update(collective_id=collective, has_side_effects=True)
    return pltpu.CompilerParams(vmem_limit_bytes=VMEM_LIMIT, **more)


def adamw(w, m, v, g):
    m = 0.9 * m + 0.1 * g
    v = 0.95 * v + 0.05 * g * g
    step = m * lax.rsqrt(v + 1e-8) + 0.1 * w
    return (w - 0.02 * step).astype(BF16), m, v


def solution(mesh):
    group, groups = mesh.shape["dp"], mesh.shape["rep"]
    chips = group // 2
    any_space = pl.BlockSpec(memory_space=pl.ANY)

    def step(x, dy, *arrays):
        weights, ms, vs = (arrays[i : i + 3] for i in (0, 3, 6))
        x, dy = x[0], dy[0]
        tokens, d = x.shape
        tiles = tokens // TILE
        rows = [(w.shape[1], w.shape[2]) for w in weights]
        ff = rows[0][1]
        d_ff = (d, ff)
        gu_blocks = jax.ShapeDtypeStruct((chips, 2, rows[0][0], 2 * ff), BF16)
        down_blocks = jax.ShapeDtypeStruct((chips, 2, *rows[2]), BF16)

        def split(g, m):
            return g.reshape(chips, 2, *rows[m])

        narrow = pl.BlockSpec((TILE, d), lambda i: (i, 0))
        broad = pl.BlockSpec((TILE, ff), lambda i: (i, 0))
        weight_specs = [whole((d, 2 * ff)), whole((ff, d))]
        tokens_d = jax.ShapeDtypeStruct((tokens, d), BF16)
        tokens_ff = jax.ShapeDtypeStruct((tokens, ff), BF16)
        tokens_t = jax.ShapeDtypeStruct((d, tokens), BF16)
        narrow_t = pl.BlockSpec((d, TILE), lambda i: (0, i))
        dma = pltpu.SemaphoreType.DMA
        h1, act0, a0, a0t, *full = pl.pallas_call(
            functools.partial(forward_kernel, chips, groups),
            grid=(tiles,),
            out_shape=[tokens_d, tokens_ff, tokens_d, tokens_t, *[gu_blocks, down_blocks] * 2],
            in_specs=[narrow, *[whole(w.shape) for w in weights]],
            out_specs=[narrow, broad, narrow, narrow_t, *[any_space] * 4],
            scratch_shapes=[pltpu.VMEM(gu_blocks.shape, BF16), pltpu.VMEM(down_blocks.shape, BF16), dma((2,))] + Gather.scratch(chips) * 2,
            compiler_params=params(1, dimension_semantics=("arbitrary",)),
            name="forward0",
        )(x, *weights)
        w0, w1 = ([full[k].reshape(d, 2 * ff), full[k + 1].reshape(ff, d)] for k in (0, 2))

        wide = jax.ShapeDtypeStruct(d_ff, BF16)
        tall = jax.ShapeDtypeStruct((ff, d), BF16)
        dh, dht, gg1, gu1, gd1 = pl.pallas_call(
            both_kernel,
            grid=(tiles,),
            out_shape=[tokens_d, tokens_t, wide, wide, tall],
            in_specs=[narrow, narrow, *weight_specs],
            out_specs=[narrow, narrow_t, whole(d_ff), whole(d_ff), whole((ff, d))],
            scratch_shapes=[pltpu.VMEM((2 * ff, d), BF16), pltpu.VMEM(d_ff, BF16), pltpu.VMEM((TILE, 2 * ff), BF16)]
            + [pltpu.VMEM((d, 2 * ff), F32)]
            + [pltpu.VMEM(d_ff, F32)],
            compiler_params=params(dimension_semantics=("arbitrary",)),
            name="both1",
        )(h1, dy, *w1)

        blocks = [jax.ShapeDtypeStruct(r, BF16) for r in rows]
        sizes = CHUNKS
        scratch = [pltpu.VMEM(d_ff, BF16), pltpu.VMEM(d_ff, F32)] + [pltpu.VMEM((d, max(sizes)), F32)] * 2
        scratch += [pltpu.VMEM((8, 128), F32)] * 2 + [pltpu.VMEM((group - 1, 8, 128), F32)] + [dma((group - 1,))] * 2
        scratch += Scatter.scratch(chips, rows[:2], True) + Scatter.scratch(chips, [rows[2]], True)
        scratch += [pltpu.VMEM((chips, 2, *rows[2]), BF16)] + Scatter.scratch(chips, [rows[2]], False)
        for size in sizes:
            block = (rows[0][0], size)
            scratch += [pltpu.VMEM((chips, 2, *block), BF16)] * 2 + Scatter.scratch(chips, [block] * 2, False)
        tiles = tokens // (2 * TILE)

        def later(i):
            return jnp.where(i < tiles, 0, lax.rem(i, tiles))

        def early(i):
            return jnp.minimum(i, tiles - 1)

        again = pl.BlockSpec((2 * TILE, d), lambda i: (later(i), 0))
        across = pl.BlockSpec((d, 2 * TILE), lambda i: (0, later(i)))
        once = [pl.BlockSpec((d, 2 * TILE), lambda i: (0, early(i))), pl.BlockSpec((2 * TILE, ff), lambda i: (early(i), 0))]
        rg0, ru0, rg1, ru1, rd1, rd0, total = pl.pallas_call(
            functools.partial(backward_kernel, chips, tiles, sizes),
            grid=((len(sizes) + 1) * tiles,),
            out_shape=[blocks[0], blocks[1], *blocks, blocks[2], jax.ShapeDtypeStruct((8, 128), F32)],
            in_specs=[again, across, again, *once, *weight_specs, *[any_space] * 3],
            out_specs=[whole(r) for r in (rows[0], rows[1], *rows, rows[2], (8, 128))],
            scratch_shapes=scratch,
            compiler_params=params(2, dimension_semantics=("arbitrary",)),
            name="backward0",
        )(a0, a0t, dh, dht, act0, *w0, split(gg1, 0), split(gu1, 1), split(gd1, 2))

        count = group * sum(w.size for w in weights)
        new = [jax.ShapeDtypeStruct(w.shape, t) for t in (BF16, F32, F32) for w in weights]
        return tuple(
            pl.pallas_call(
                functools.partial(step_kernel, count),
                out_shape=new,
                in_specs=[whole()] * 16,
                out_specs=[whole()] * 9,
                compiler_params=params(),
                name="adamw",
            )(total, *weights, *ms, *vs, rg0, rg1, ru0, ru1, rd0, rd1)
        )

    states, cut = P(("rep", "dp"), None, None), P(None, "dp", None)
    return jax.shard_map(
        step,
        mesh=mesh,
        in_specs=(states, states) + (cut,) * 9,
        out_specs=(P("rep", "dp", None),) * 9,
        check_vma=False,
    )
```

```python
import functools
import math

import jax
import jax.numpy as jnp
from jax import lax
from jax.experimental import pallas as pl
from jax.experimental.pallas import tpu as pltpu
from jax.sharding import PartitionSpec as P

F32, BF16 = jnp.float32, jnp.bfloat16
TILE = 512
VMEM_LIMIT = 60 << 20
MESH = pl.DeviceIdType.MESH


def dot(a, b):
    return jnp.dot(a, b, preferred_element_type=F32)


def norm_parts(h):
    wide = h.astype(F32)
    scale = lax.rsqrt(jnp.mean(wide * wide, -1, keepdims=True) + 1e-6)
    return wide, scale, (wide * scale).astype(BF16)


def sigmoid(x):
    return 0.5 * jnp.tanh(0.5 * x) + 0.5


class Place:
    def __init__(self, chips, groups=None):
        self.dp = me = lax.axis_index("dp")
        if groups is not None:
            rep, length = lax.axis_index("rep"), math.isqrt(groups)
            x, y = rep // length, rep % length
            self.parity = (x + y) % 2
            self.across = ((x + 1 - 2 * (x % 2)) * length + y, x * length + y + 1 - 2 * (y % 2))
        self.chips, self.half = chips, chips // 2
        self.z, self.c = me // 2, me % 2
        self.sibling = self.z * 2 + 1 - self.c

    def chip(self, offset):
        return lax.rem(self.z + offset + 2 * self.chips, self.chips)

    def beside(self, direction):
        return self.chip(direction) * 2 + self.c


def ident(device, group=None):
    return {"dp": device} if group is None else {"rep": group, "dp": device}


def meet(devices):
    barrier = pltpu.get_barrier_semaphore()
    for device in devices:
        pl.semaphore_signal(barrier, inc=1, device_id=ident(*device), device_id_type=MESH)
    pl.semaphore_wait(barrier, len(devices))


def remote(src, dst, send, recv, device, group=None):
    return pltpu.make_async_remote_copy(src_ref=src, dst_ref=dst, send_sem=send, recv_sem=recv, device_id=ident(device, group), device_id_type=MESH)


DIRECTIONS = (1, -1)


class Gather:
    PIECES = 4
    SIGNS = (1, -1, 1, -1)

    def __init__(self, place, layer, shards, gu, down, sems):
        self.p, self.shards, self.gu, self.down = place, [s.at[layer] for s in shards], gu, down
        self.ring_send, self.ring_recv, self.cross_send, self.cross_recv, self.side_send, self.side_recv, self.own_sem = sems
        self.rows, self.ff = self.shards[0].shape
        self.d = self.shards[2].shape[1]

    @staticmethod
    def scratch(chips):
        ring, dma = 2 * (chips // 2) * Gather.PIECES, pltpu.SemaphoreType.DMA
        return [dma((ring,)), dma((ring,)), dma((Gather.PIECES,)), dma((ring,)), dma((2,)), dma((2,)), dma((3,))]

    def goes(self, direction, step, m):
        return step < self.p.half - 1 or self.SIGNS[m] == direction

    def part(self, m, parity):
        if m < 2:
            half = self.rows // 2
            return pl.ds(pl.multiple_of(parity * half, half), half), slice(None)
        quarter = self.d // 4
        return slice(None), pl.ds(pl.multiple_of((2 * parity + m - 2) * quarter, quarter), quarter)

    def block(self, m, chip, core):
        return self.down.at[chip, core] if m >= 2 else self.gu.at[chip, core, :, m * self.ff : (m + 1) * self.ff]

    def piece(self, m, chip, parity):
        return self.block(m, chip, self.p.c).at[self.part(m, parity)]

    def source(self, direction, step, m, parity):
        if step == 0:
            return self.shards[min(m, 2)].at[self.part(m, parity)]
        return self.piece(m, self.p.chip(-direction * step), parity)

    def index(self, direction, step, m):
        return ((direction < 0) * self.p.half + step) * self.PIECES + m

    def ring(self, direction, step, m):
        p, k = self.p, self.index(direction, step, m)
        place = self.piece(m, p.chip(-direction * step), p.parity)
        return remote(self.source(direction, step, m, p.parity), place, self.ring_send.at[k], self.ring_recv.at[k], p.beside(direction))

    def cross(self, direction, step, m):
        p, k = self.p, self.index(direction, step, m)
        place = self.piece(m, p.chip(-direction * (step + 1)), p.parity)
        return remote(place, place, self.cross_send.at[m], self.cross_recv.at[k], p.dp, p.across[m % 2])

    def side(self, ref, m):
        return remote(ref, ref, self.side_send.at[m // 2], self.side_recv.at[m // 2], self.p.sibling)

    def own(self, m):
        return pltpu.make_async_copy(self.shards[m], self.block(m, self.p.z, self.p.c), self.own_sem.at[m])

    def start(self):
        p = self.p
        for m in range(self.PIECES):
            for direction in DIRECTIONS:
                if self.goes(direction, 0, m):
                    self.ring(direction, 0, m).start()
        for m in range(3):
            self.own(m).start()
            place = self.block(m, p.z, p.c)
            remote(self.shards[m], place, self.side_send.at[m // 2], self.side_recv.at[m // 2], p.sibling).start()

    def step(self, step, m):
        p = self.p
        for direction in DIRECTIONS:
            if self.goes(direction, step - 1, m):
                self.ring(direction, step - 1, m).wait_recv()
                if step < p.half and self.goes(direction, step, m):
                    self.ring(direction, step, m).start()
                self.cross(direction, step - 1, m).start()
                self.side(self.piece(m, p.chip(-direction * step), p.parity), m).start()

    def crossed(self, step, m):
        p = self.p
        for direction in DIRECTIONS:
            if self.goes(direction, step - 1, m):
                chip = p.chip(-direction * step)
                k = self.index(direction, step - 1, m)
                place = self.piece(m, chip, 1 - p.parity)
                remote(place, place, self.cross_send.at[m], self.cross_recv.at[k], p.dp, p.across[m % 2]).wait_recv()
                self.side(place, m).start()

    def finish(self):
        p = self.p
        for m in range(3):
            self.own(m).wait()
        for m, ref in ((0, self.gu), (2, self.down)):
            self.side(ref.at[:, 0], m).wait()
        for m in range(self.PIECES):
            sent = self.block(m, slice(0, p.chips - 1), 0).at[(slice(None), *self.first(m))]
            remote(sent, sent, self.cross_send.at[m], self.cross_recv.at[0], p.dp, p.across[m % 2]).wait_send()
            for direction in DIRECTIONS:
                for step in range(p.half):
                    if self.goes(direction, step, m):
                        self.ring(direction, step, m).wait_send()

    def first(self, m):
        return (slice(0, self.rows // 2), slice(None)) if m < 2 else (slice(None), slice(0, self.d // 4))


class Scatter:
    def __init__(self, place, terms, signs, scratch, in_hbm):
        self.p, self.terms, self.signs, self.in_hbm, n = place, terms, signs, in_hbm, len(terms)
        scratch = list(scratch)
        take = lambda k: [scratch.pop(0) for _ in range(k)]
        self.other, self.sent, self.came = take(n), take(n), take(n)
        self.own = take(n) if in_hbm else None
        self.pair_send, self.pair_recv, self.ring_send, self.ring_recv, self.own_sem = scratch

    @staticmethod
    def scratch(chips, shapes, in_hbm):
        steps, n, dma = chips // 2, len(shapes), pltpu.SemaphoreType.DMA
        blocks = [pltpu.VMEM((chips, *shape), BF16) for shape in shapes]
        slots = [pltpu.VMEM((2 * steps, *shape), BF16) for shape in shapes]
        return blocks + slots * 2 + blocks * in_hbm + [dma((n,)), dma((n,)), dma((2 * steps * n,)), dma((2 * steps * n,)), dma((n,))]

    def local(self, m):
        return pltpu.make_async_copy(self.terms[m].at[:, self.p.c], self.own[m], self.own_sem.at[m])

    def pair(self, m):
        return remote(self.terms[m].at[:, 1 - self.p.c], self.other[m], self.pair_send.at[m], self.pair_recv.at[m], self.p.sibling)

    def goes(self, direction, step, m):
        return step > 0 or self.signs[m] == direction

    def slot(self, direction, step):
        return (direction < 0) * self.p.half + step

    def ring(self, direction, step, m):
        slot = self.slot(direction, step)
        k = slot * len(self.terms) + m
        return remote(self.sent[m].at[slot], self.came[m].at[slot], self.ring_send.at[k], self.ring_recv.at[k], self.p.beside(direction))

    def exchange(self):
        for m in range(len(self.terms)):
            self.pair(m).start()
            if self.in_hbm:
                self.local(m).start()

    def mine(self, m, t):
        own = self.own[m][t] if self.in_hbm else self.terms[m][t, self.p.c]
        return own.astype(F32) + self.other[m][t].astype(F32)

    def step(self, step):
        for m in range(len(self.terms)):
            if step == 0:
                if self.in_hbm:
                    self.local(m).wait()
                self.pair(m).wait_recv()
            for direction in DIRECTIONS:
                if not self.goes(direction, step, m):
                    continue
                value = self.mine(m, self.p.chip(direction * (self.p.half - step)))
                if step > 0 and self.goes(direction, step - 1, m):
                    self.ring(direction, step - 1, m).wait_recv()
                    value = value + self.came[m][self.slot(direction, step - 1)].astype(F32)
                self.sent[m][self.slot(direction, step)] = value.astype(BF16)
                self.ring(direction, step, m).start()

    def result(self, m):
        last = self.p.half - 1
        value = self.mine(m, self.p.z)
        for direction in DIRECTIONS:
            self.ring(direction, last, m).wait_recv()
            value = value + self.came[m][self.slot(direction, last)].astype(F32)
        return value.astype(BF16)

    def finish(self):
        for m in range(len(self.terms)):
            self.pair(m).wait_send()
            for direction in DIRECTIONS:
                for step in range(self.p.half):
                    if self.goes(direction, step, m):
                        self.ring(direction, step, m).wait_send()


CHUNKS = (512, 512, 384)
SCHEDULE = {
    "first": (2, 3, 5, 7),
    "second": (2, 4, 6, 8),
    "chunk0": (4, 5, 6, 8, 10),
    "chunk1": (8, 9, 11),
}


def forward_kernel(chips, groups, x, s0, s1, s2, h_out, act_out, a_out, at_out, w0gu, w0d, w1gu, w1d, gu, down, keep_sem, *sems):
    i, n = pl.program_id(0), pl.num_programs(0)
    place = Place(chips, groups)
    ff = s0.shape[2]
    d = x.shape[1]
    half = len(sems) // 2
    one = Gather(place, 0, (s0, s1, s2), gu, down, sems[:half])
    two = Gather(place, 1, (s0, s1, s2), w1gu, w1d, sems[half:])
    keep = [pltpu.make_async_copy(src, dst, keep_sem.at[k]) for k, (src, dst) in enumerate(((gu, w0gu), (down, w0d)))]
    last = place.half
    pieces = range(Gather.PIECES)

    @pl.when(i == 0)
    def _():
        meet([(place.sibling,), (place.beside(1),), (place.beside(-1),), *[(place.dp, group) for group in place.across]])
        one.start()
        for step in range(1, last + 1):
            for m in pieces:
                one.step(step, m)
                if step > 1:
                    one.crossed(step - 1, m)
        two.start()
        for m in pieces:
            one.crossed(last, m)
        one.finish()
        for copy in keep:
            copy.start()

    for step in range(1, last + 1):
        for late, some in enumerate(((0, 1), (2, 3))):

            @pl.when(i == min(2 * step - 1 + late, 2 * last - 1))
            def _(step=step, some=some):
                for m in some:
                    two.step(step, m)
                    if step > 1:
                        two.crossed(step - 1, m)

    h = x[...]
    _, _, a = norm_parts(h)
    a_out[...] = a
    at_out[...] = a.T
    both = dot(a, gu[...].reshape(d, 2 * ff))
    gate, up = both[:, :ff], both[:, ff:]
    act = (gate * sigmoid(gate) * up).astype(BF16)
    act_out[...] = act
    out = dot(act, down[...].reshape(ff, d)).astype(BF16)
    h_out[...] = (h.astype(F32) + out.astype(F32)).astype(BF16)

    @pl.when(i == n - 1)
    def _():
        for m in pieces:
            two.crossed(last, m)
        two.finish()
        for copy in keep:
            copy.wait()


def act_backward(gate, up, by_act):
    by_act = by_act.astype(BF16).astype(F32)
    sig = sigmoid(gate)
    silu = gate * sig
    act = (silu * up).astype(BF16)
    by_up = (by_act * silu).astype(BF16)
    by_gate = (by_act * up * (sig + silu * (1.0 - sig))).astype(BF16)
    return act, by_gate, by_up


def both_kernel(h, dy, act0, wgu, wd, dh_out, gg, gu, gd, gd0, wgut, wdt, by_gu, agu, ad, ad0):
    i, n = pl.program_id(0), pl.num_programs(0)
    ff = wd.shape[0]

    @pl.when(i == 0)
    def _():
        wgut[...] = wgu[...].T
        wdt[...] = wd[...].T
        for acc in (agu, ad, ad0):
            acc[...] = jnp.zeros_like(acc)

    by_out = dy[...]
    wide, scale, a = norm_parts(h[...])
    both = dot(a, wgu[...])
    act, by_gate, by_up = act_backward(both[:, :ff], both[:, ff:], dot(by_out, wdt[...]))
    by_gu[:, :ff] = by_gate
    by_gu[:, ff:] = by_up
    by_a = dot(by_gu[...], wgut[...]).astype(BF16).astype(F32)
    agu[...] += dot(a.T, by_gu[...])
    ad[...] += dot(by_out.T, act)
    by_wide = by_a * scale - wide * (scale * scale * scale * jnp.mean(by_a * wide, -1, keepdims=True))
    by_h = (by_out.astype(F32) + by_wide.astype(BF16).astype(F32)).astype(BF16)
    dh_out[...] = by_h
    ad0[...] += dot(by_h.T, act0[...])

    @pl.when(i == n - 1)
    def _():
        gg[...] = agu[:, :ff].astype(BF16)
        gu[...] = agu[:, ff:].astype(BF16)
        gd[...] = ad[...].astype(BF16).T
        gd0[...] = ad0[...].astype(BF16).T


def add_up(squares, g):
    g = g.astype(F32)
    g = (g * g).reshape(g.shape[0] // 8, 8, g.shape[1]).sum(0)
    return squares + sum(g[:, k : k + 128] for k in range(0, g.shape[1], 128))


def backward_kernel(chips, tiles, sizes, a, at, dh, wgu, wd, t0, t1, t2, t3, rg, ru, rg1, ru1, rd1, rd0, total, wdt, ag, au, squares, part, parts, part_send, part_recv, *scratch):
    i = pl.program_id(0)
    place = Place(chips)
    group = 2 * chips
    me = lax.axis_index("dp")
    ff = wd.shape[0]
    scratch = list(scratch)
    take = lambda k: [scratch.pop(0) for _ in range(k)]
    hbm_count, chunk_count = 4 * 2 + 5, 3 * 2 + 5
    first = Scatter(place, (t0, t1), (1, -1), take(hbm_count), True)
    second = Scatter(place, (t2, t3), (1, -1), take(hbm_count), True)
    chunks = []
    for _ in sizes:
        terms = take(2)
        chunks.append(Scatter(place, terms, (1, -1), take(chunk_count), False))
    steps = place.half
    starts = [sum(sizes[:k]) for k in range(len(sizes))]

    def settle(scatter, outs):
        sums = squares[...]
        for m, out in enumerate(outs):
            value = scatter.result(m)
            out[...] = value
            sums = add_up(sums, value)
        squares[...] = sums
        scatter.finish()

    def chunk_outs(k):
        return [r.at[:, starts[k] : starts[k] + sizes[k]] for r in (rg, ru)]

    events = []
    for name, scatter in (("first", first), ("second", second)):
        times = SCHEDULE[name]
        events += [(times[s], functools.partial(scatter.step, s)) for s in range(steps)]
    for k in range(len(sizes) - 1):
        times = SCHEDULE[f"chunk{k}"]
        for s in range(len(times) - 1):
            events.append((times[s + 1], functools.partial(chunks[k].step, s) if s < steps else functools.partial(settle, chunks[k], chunk_outs(k))))

    def clear():
        ag[...] = jnp.zeros_like(ag)
        au[...] = jnp.zeros_like(au)

    @pl.when(i == 0)
    def _():
        others = [lax.rem(me + k, group) for k in range(1, group)]
        meet([(other,) for other in others])
        first.exchange()
        second.exchange()
        squares[...] = jnp.zeros_like(squares)
        wdt[...] = wd[...].T
        clear()

    for when in sorted({when for when, _ in events}):

        @pl.when(i == when)
        def _(now=when):
            for when, act in events:
                if when == now:
                    act()

    for k, size in enumerate(sizes):

        @pl.when(i // tiles == k)
        def _(k=k, size=size):
            cols = slice(starts[k], starts[k] + size)
            by_out = dh[...]
            gate, up = dot(a[...], wgu[:, cols]), dot(a[...], wgu[:, ff + cols.start : ff + cols.stop])
            _, by_gate, by_up = act_backward(gate, up, dot(by_out, wdt[:, cols]))
            ag[:, :size] += dot(at[...], by_gate)
            au[:, :size] += dot(at[...], by_up)

        @pl.when(i == (k + 1) * tiles - 1)
        def _(k=k, size=size):
            for term, acc in zip(chunks[k].terms, (ag, au)):
                term[...] = acc[:, :size].astype(BF16).reshape(term.shape)
            chunks[k].exchange()
            clear()

    @pl.when(i == len(sizes) * tiles - 1)
    def _():
        done = [len(SCHEDULE[f"chunk{k}"]) - 1 for k in range(len(sizes) - 1)] + [0]
        for s in range(steps):
            for k, chunk in reversed(list(enumerate(chunks))):
                if done[k] <= steps and done[k] + s < steps:
                    chunk.step(done[k] + s)
                elif done[k] <= steps and done[k] + s == steps:
                    settle(chunk, chunk_outs(k))
            if s == steps - 2:
                settle(first, (rg1, ru1))
            if s == steps - 1:
                settle(second, (rd1, rd0))
        settle(chunks[-1], chunk_outs(len(sizes) - 1))
        part[...] = squares[...]
        copies = [remote(part, parts.at[group - k - 1], part_send.at[k - 1], part_recv.at[group - k - 1], lax.rem(me + k, group)) for k in range(1, group)]
        for copy in copies:
            copy.start()
        sums = squares[...]
        for k in range(1, group):
            remote(part, parts.at[k - 1], part_send.at[k - 1], part_recv.at[k - 1], lax.rem(me + k, group)).wait_recv()
            sums = sums + parts[k - 1]
        for copy in copies:
            copy.wait_send()
        total[...] = sums


def step_kernel(count, total, *refs):
    ws, ms, vs, gs, outs = refs[:3], refs[3:6], refs[6:9], refs[9:15], refs[15:]
    squares = jnp.sum(jnp.sum(total[...], 0, keepdims=True), 1, keepdims=True)
    factor = jnp.minimum(1.0, 0.5 * lax.rsqrt(squares / count + 1e-30))
    for k in range(3):
        for layer in range(2):
            g = gs[2 * k + layer][...].astype(F32) * factor
            w, m, v = adamw(ws[k][layer].astype(F32), ms[k][layer], vs[k][layer], g)
            outs[k][layer], outs[3 + k][layer], outs[6 + k][layer] = w, m, v


def whole(shape=None):
    return pl.BlockSpec(memory_space=pltpu.VMEM) if shape is None else pl.BlockSpec(shape, lambda i: (0,) * len(shape), pipeline_mode=pl.Buffered(1))


def params(collective=None, **more):
    if collective is not None:
        more.update(collective_id=collective, has_side_effects=True)
    return pltpu.CompilerParams(vmem_limit_bytes=VMEM_LIMIT, **more)


def adamw(w, m, v, g):
    m = 0.9 * m + 0.1 * g
    v = 0.95 * v + 0.05 * g * g
    step = m * lax.rsqrt(v + 1e-8) + 0.1 * w
    return (w - 0.02 * step).astype(BF16), m, v


def solution(mesh):
    group, groups = mesh.shape["dp"], mesh.shape["rep"]
    chips = group // 2
    any_space = pl.BlockSpec(memory_space=pl.ANY)

    def step(x, dy, *arrays):
        weights, ms, vs = (arrays[i : i + 3] for i in (0, 3, 6))
        x, dy = x[0], dy[0]
        tokens, d = x.shape
        tiles = tokens // TILE
        rows = [(w.shape[1], w.shape[2]) for w in weights]
        ff = rows[0][1]
        d_ff = (d, ff)
        gu_blocks = jax.ShapeDtypeStruct((chips, 2, rows[0][0], 2 * ff), BF16)
        down_blocks = jax.ShapeDtypeStruct((chips, 2, *rows[2]), BF16)

        def split(g, m):
            return g.reshape(chips, 2, *rows[m])

        narrow = pl.BlockSpec((TILE, d), lambda i: (i, 0))
        broad = pl.BlockSpec((TILE, ff), lambda i: (i, 0))
        weight_specs = [whole((d, 2 * ff)), whole((ff, d))]
        tokens_d = jax.ShapeDtypeStruct((tokens, d), BF16)
        tokens_ff = jax.ShapeDtypeStruct((tokens, ff), BF16)
        dma = pltpu.SemaphoreType.DMA
        h1, act0, a0, a0t, *full = pl.pallas_call(
            functools.partial(forward_kernel, chips, groups),
            grid=(tiles,),
            out_shape=[tokens_d, tokens_ff, tokens_d, jax.ShapeDtypeStruct((d, tokens), BF16), *[gu_blocks, down_blocks] * 2],
            in_specs=[narrow, *[whole(w.shape) for w in weights]],
            out_specs=[narrow, broad, narrow, pl.BlockSpec((d, TILE), lambda i: (0, i)), *[any_space] * 4],
            scratch_shapes=[pltpu.VMEM(gu_blocks.shape, BF16), pltpu.VMEM(down_blocks.shape, BF16), dma((2,))] + Gather.scratch(chips) * 2,
            compiler_params=params(1, dimension_semantics=("arbitrary",)),
            name="forward0",
        )(x, *weights)
        w0, w1 = ([full[k].reshape(d, 2 * ff), full[k + 1].reshape(ff, d)] for k in (0, 2))

        wide = jax.ShapeDtypeStruct(d_ff, BF16)
        tall = jax.ShapeDtypeStruct((ff, d), BF16)
        dh, gg1, gu1, gd1, gd0 = pl.pallas_call(
            both_kernel,
            grid=(tiles,),
            out_shape=[tokens_d, wide, wide, tall, tall],
            in_specs=[narrow, narrow, broad, *weight_specs],
            out_specs=[narrow, whole(d_ff), whole(d_ff), whole((ff, d)), whole((ff, d))],
            scratch_shapes=[pltpu.VMEM((2 * ff, d), BF16), pltpu.VMEM(d_ff, BF16), pltpu.VMEM((TILE, 2 * ff), BF16)]
            + [pltpu.VMEM((d, 2 * ff), F32)]
            + [pltpu.VMEM(d_ff, F32)] * 2,
            compiler_params=params(dimension_semantics=("arbitrary",)),
            name="both1",
        )(h1, dy, act0, *w1)

        blocks = [jax.ShapeDtypeStruct(r, BF16) for r in rows]
        sizes = CHUNKS
        scratch = [pltpu.VMEM(d_ff, BF16)] + [pltpu.VMEM((d, max(sizes)), F32)] * 2
        scratch += [pltpu.VMEM((8, 128), F32)] * 2 + [pltpu.VMEM((group - 1, 8, 128), F32)] + [dma((group - 1,))] * 2
        scratch += Scatter.scratch(chips, rows[:2], True) + Scatter.scratch(chips, [rows[2]] * 2, True)
        for size in sizes:
            block = (rows[0][0], size)
            scratch += [pltpu.VMEM((chips, 2, *block), BF16)] * 2 + Scatter.scratch(chips, [block] * 2, False)
        tiles = tokens // (2 * TILE)
        again = pl.BlockSpec((2 * TILE, d), lambda i: (lax.rem(i, tiles), 0))
        across = pl.BlockSpec((d, 2 * TILE), lambda i: (0, lax.rem(i, tiles)))
        rg0, ru0, rg1, ru1, rd1, rd0, total = pl.pallas_call(
            functools.partial(backward_kernel, chips, tiles, sizes),
            grid=(len(sizes) * tiles,),
            out_shape=[blocks[0], blocks[1], *blocks, blocks[2], jax.ShapeDtypeStruct((8, 128), F32)],
            in_specs=[again, across, again, *weight_specs, *[any_space] * 4],
            out_specs=[whole(r) for r in (rows[0], rows[1], *rows, rows[2], (8, 128))],
            scratch_shapes=scratch,
            compiler_params=params(2, dimension_semantics=("arbitrary",)),
            name="backward0",
        )(a0, a0t, dh, *w0, split(gg1, 0), split(gu1, 1), split(gd1, 2), split(gd0, 2))

        count = group * sum(w.size for w in weights)
        new = [jax.ShapeDtypeStruct(w.shape, t) for t in (BF16, F32, F32) for w in weights]
        return tuple(
            pl.pallas_call(
                functools.partial(step_kernel, count),
                out_shape=new,
                in_specs=[whole()] * 16,
                out_specs=[whole()] * 9,
                compiler_params=params(),
                name="adamw",
            )(total, *weights, *ms, *vs, rg0, rg1, ru0, ru1, rd0, rd1)
        )

    states, cut = P(("rep", "dp"), None, None), P(None, "dp", None)
    return jax.shard_map(
        step,
        mesh=mesh,
        in_specs=(states, states) + (cut,) * 9,
        out_specs=(P("rep", "dp", None),) * 9,
        check_vma=False,
    )
```
